32 devices in a mesh: ctx: 8 (over y, x, core), mp: 4 (over z).
Axes of the slice: x: 2, y: 2, z: 4, core: 2. Of those that a mesh axis runs over, the one named last changes fastest.
Arguments:
- tokens: bfloat16 [4096, 8192], P('ctx', 'mp'), may hold values from -12 to 12
- norm_gain: bfloat16 [8192], replicated, may hold values from 0.099609375 to 1.8984375
- router_weight: bfloat16 [8192], replicated, may hold values from -0.0625 to 0.0625
- query_weight: bfloat16 [8192, 4096], P('ctx', 'mp'), may hold values from -2 to 2
- key_weight: bfloat16 [8192, 1024], P('ctx', 'mp'), may hold values from -1 to 1
- value_weight: bfloat16 [8192, 1024], P('ctx', 'mp'), may hold values from -0.0625 to 0.0625
- out_weight: bfloat16 [4096, 8192], P('mp', 'ctx'), may hold values from -0.1875 to 0.1875
- mlp_gain: bfloat16 [8192], P('mp'), may hold values from 0.099609375 to 1.8984375
- gate_weight: bfloat16 [8192, 28672], P('mp', 'ctx'), may hold values from -0.0625 to 0.0625
- up_weight: bfloat16 [8192, 28672], P('mp', 'ctx'), may hold values from -0.0625 to 0.0625
- down_weight: bfloat16 [28672, 8192], P('ctx', 'mp'), may hold values from -0.0625 to 0.0625
- destination: int32 [4096], P('ctx'), may hold values from -1 to 511, as said below
- kept_pos: int32 [512], P('ctx'), may hold values from 0 to 4095, as said below
Outputs:
- layer_out: bfloat16 [4096, 8192], P('ctx', 'mp')
The draws below stay inside these ranges and needn't reach their ends.
Inputs may be any that keep to these rules, and one draw needn't show every extreme that they name: A token that skips the block has -1. The kept tokens, counted in sequence order as k = 0, 1, ..., 511, have destination (k mod 8) * 64 + (k div 8): owner k mod 8, slot k div 8 of that owner. Each shard of 512 tokens keeps from 32 to 96 tokens, and in every draw some shard keeps exactly 96; so at most 12 kept tokens of one shard have one owner, and that most is reached in every draw. kept_pos[destination[t]] = t for every kept token t.
All inputs are finite; a program needn't handle non-finite values.
Results may differ from the reference program's by a relative error of at most 0.0055.
Values may be sent and summed in bfloat16 or wider, within the bound.
No kernel may reach another device: no remote copies, remote signals or barrier semaphores. Data moves between devices by JAX's collectives and lax.ppermute only.
A program may use at most 128 MiB of HBM per device.

```python
import jax
import jax.numpy as jnp
from jax import lax

D = 8192
FF = 28672
HEADS = 32
KV_HEADS = 8
HEAD_DIM = 128
TOK_DEV = 512
TOKENS = 4096
KEPT_DEV = 64
KEPT = 512


def kept_layout(key):
    shard_count = TOKENS // TOK_DEV
    pair_count = shard_count // 2
    spread_rows = KEPT_DEV // 2
    key_offset, key_forced, key_sign, key_order = jax.random.split(jax.random.fold_in(key, 41), 4)
    offsets = jax.random.randint(key_offset, (pair_count,), -spread_rows, spread_rows + 1)
    forced = jax.random.randint(key_forced, (), 0, pair_count)
    sign_value = 2 * jax.random.randint(key_sign, (), 0, 2) - 1
    offsets = jnp.where(jnp.arange(pair_count) == forced, spread_rows * sign_value, offsets)
    counts = jnp.concatenate([KEPT_DEV + offsets, (KEPT_DEV - offsets)[::-1]])
    orders = jax.vmap(lambda subkey: jax.random.permutation(subkey, TOK_DEV))(jax.random.split(key_order, shard_count))
    is_kept = (orders < counts[:, None]).reshape(-1)
    kept_rank = jnp.cumsum(is_kept.astype(jnp.int32)) - 1
    destination = jnp.where(is_kept, kept_rank % shard_count * KEPT_DEV + kept_rank // shard_count, -1).astype(jnp.int32)
    targets = jnp.where(is_kept, destination, KEPT).astype(jnp.int32)
    kept_pos = jnp.zeros((KEPT,), jnp.int32).at[targets].set(jnp.arange(TOKENS, dtype=jnp.int32), mode='drop')
    rank_slots = jnp.where(is_kept, kept_rank, KEPT).astype(jnp.int32)
    ranked = jnp.zeros((KEPT,), jnp.int32).at[rank_slots].set(jnp.arange(TOKENS, dtype=jnp.int32), mode='drop')
    return (destination, kept_pos, ranked)


def plant_sign(key):
    coins = jax.random.randint(jax.random.fold_in(key, 53), (D,), 0, 2)
    return (2 * coins - 1).astype(jnp.float32)


def plant_mask(width):
    within = jnp.arange(width, dtype=jnp.int32) % HEAD_DIM
    half_dim = HEAD_DIM // 2
    return (within % half_dim >= half_dim - 2).astype(jnp.float32)


def drawn_weight(key, salt, width, spread):
    base = jnp.clip(jax.random.normal(jax.random.fold_in(key, salt), (D, width), jnp.float32), -4.0, 4.0) * spread
    lift = jnp.sqrt(80.0) * HEAD_DIM ** 0.25 / D
    return (base + lift * plant_sign(key)[:, None] * plant_mask(width)[None, :]).astype(jnp.bfloat16)


def draw_destination(key, part):
    return kept_layout(key)[0]


def draw_kept_pos(key, part):
    return kept_layout(key)[1]


def draw_query_weight(key, part):
    return drawn_weight(key, 73, HEADS * HEAD_DIM, (D // 16) ** (-0.5))


def draw_key_weight(key, part):
    return drawn_weight(key, 79, KV_HEADS * HEAD_DIM, D ** (-0.5))


def draw_tokens(key, part):
    ranked = kept_layout(key)[2]
    noise_key = jax.random.fold_in(key, 61)
    ramp = jnp.arange(D, dtype=jnp.float32) / max(D - 1, 1)
    noise = jnp.clip(jax.random.normal(noise_key, (TOKENS, D), jnp.float32), -3.5, 3.5)
    column_scale = jnp.power(2.25, ramp)
    planted = jnp.arange(8, dtype=jnp.int32)
    planted_ranks = (planted + 1) * KEPT // 9
    strengths = 0.5 + 0.15 * (planted // 2).astype(jnp.float32)
    strength = jnp.zeros((TOKENS,), jnp.float32).at[ranked[planted_ranks]].set(strengths)
    lifted = strength[:, None] * plant_sign(key)[None, :] + jnp.sqrt(1.0 - strength * strength)[:, None] * noise
    return (lifted * column_scale[None, :]).astype(jnp.bfloat16)


def block_scale(rng, extent, pieces, least, top_value):
    level = 1.0
    for dim, blocks in pieces:
        heights = jax.random.uniform(jax.random.fold_in(jax.random.fold_in(rng, 6), dim), (blocks,), jnp.float32, least / len(pieces), top_value / len(pieces))
        level = level * jnp.repeat(jnp.exp(heights), extent[dim] // blocks).reshape((-1,) + (1,) * (len(extent) - 1 - dim))
    return level


def centred(own_key, shape, deviation, reach, cuts=(), held_as=jnp.bfloat16):
    level = block_scale(own_key, shape, cuts, -0.22, 0.18) if cuts else 1.0
    drawn = jax.random.normal(own_key, shape, jnp.float32) * deviation * level
    return jnp.minimum(jnp.maximum(drawn, -reach), reach).astype(held_as)


def setup_inputs(seed: int = 0) -> dict:
    streams_of = jax.random.split(jax.random.key(seed), 14)
    return {
        "tokens": draw_tokens(jax.random.fold_in(streams_of[13], 71), 0),
        "norm_gain": jnp.clip(1.0 + 0.18 * jax.random.normal(streams_of[1], (D,), jnp.float32), 0.099609375, 1.8984375).astype(jnp.bfloat16),
        "router_weight": centred(streams_of[2], (D,), D ** -0.5, 0.0625),
        "query_weight": draw_query_weight(jax.random.fold_in(streams_of[13], 71), 0),
        "key_weight": draw_key_weight(jax.random.fold_in(streams_of[13], 71), 0),
        "value_weight": centred(streams_of[5], (D, KV_HEADS * HEAD_DIM), D ** -0.5, 0.0625, ((0, 8), (1, 4))),
        "out_weight": centred(streams_of[6], (HEADS * HEAD_DIM, D), (HEADS * HEAD_DIM // 4) ** -0.5, 0.1875, ((0, 4), (1, 8))),
        "mlp_gain": jnp.clip(1.0 + 0.18 * jax.random.normal(streams_of[7], (D,), jnp.float32), 0.099609375, 1.8984375).astype(jnp.bfloat16),
        "gate_weight": centred(streams_of[8], (D, FF), D ** -0.5, 0.0625, ((0, 4), (1, 8))),
        "up_weight": centred(streams_of[9], (D, FF), D ** -0.5, 0.0625, ((0, 4), (1, 8))),
        "down_weight": centred(streams_of[10], (FF, D), (FF // 4) ** -0.5, 0.0625, ((0, 8), (1, 4))),
        "destination": draw_destination(jax.random.fold_in(streams_of[13], 71), 0),
        "kept_pos": draw_kept_pos(jax.random.fold_in(streams_of[13], 71), 0),
    }


def rotate(values, positions):
    half_dim = values.shape[-1] // 2
    exponent = jnp.arange(half_dim, dtype=jnp.float32) * (2.0 / values.shape[-1])
    frequency = 500000.0 ** (-exponent)
    angles = positions.astype(jnp.float32)[:, None] * frequency[None, :]
    cosine = jnp.cos(angles)[:, None, :]
    sine_part = jnp.sin(angles)[:, None, :]
    first_half = values[..., :half_dim]
    second_half = values[..., half_dim:]
    return jnp.concatenate([first_half * cosine - second_half * sine_part, second_half * cosine + first_half * sine_part], axis=-1)

def reference(tokens, norm_gain, router_weight, query_weight, key_weight, value_weight, out_weight, mlp_gain, gate_weight, up_weight, down_weight, destination, kept_pos):
    slot_count = kept_pos.shape[0]
    group_size = HEADS // KV_HEADS
    targets = jnp.where(destination >= 0, destination, slot_count).astype(jnp.int32)
    sources = jnp.zeros((slot_count,), jnp.int32).at[targets].set(jnp.arange(destination.shape[0], dtype=jnp.int32), mode='drop')
    gathered = tokens[sources]
    raw_rows = gathered.astype(jnp.float32)
    mean_square = lax.optimization_barrier(jnp.mean(raw_rows * raw_rows, axis=-1, keepdims=True))
    normed = (raw_rows * lax.rsqrt(mean_square + 1e-05) * norm_gain.astype(jnp.float32)).astype(jnp.bfloat16)
    router_score = jax.nn.sigmoid(jnp.dot(gathered, router_weight, preferred_element_type=jnp.float32))
    queries = jnp.dot(normed, query_weight, preferred_element_type=jnp.float32).reshape(slot_count, HEADS, HEAD_DIM)
    queries = rotate(queries, kept_pos).astype(jnp.bfloat16)
    keys_all = jnp.dot(normed, key_weight, preferred_element_type=jnp.float32).reshape(slot_count, KV_HEADS, HEAD_DIM)
    keys_all = rotate(keys_all, kept_pos).astype(jnp.bfloat16)
    values_all = jnp.dot(normed, value_weight, preferred_element_type=jnp.float32).reshape(slot_count, KV_HEADS, HEAD_DIM).astype(jnp.bfloat16)
    allowed = kept_pos[None, :] <= kept_pos[:, None]
    softmax_scale = HEAD_DIM ** (-0.5)

    def one_group(operands):
        group_queries, group_keys, group_values = operands
        scores = jnp.einsum('qgd,kd->gqk', group_queries.astype(jnp.float32), group_keys.astype(jnp.float32)) * softmax_scale
        scores = jnp.where(allowed[None], scores, -1e+30)
        row_peak = lax.optimization_barrier(jnp.max(scores, axis=-1, keepdims=True))
        weights = jnp.where(allowed[None], jnp.exp(scores - row_peak), 0.0)
        mixed = jnp.einsum('gqk,kd->qgd', weights, group_values.astype(jnp.float32))
        return mixed / lax.optimization_barrier(jnp.sum(weights, axis=-1)).transpose(1, 0)[..., None]
    grouped = queries.reshape(slot_count, KV_HEADS, group_size, HEAD_DIM).transpose(1, 0, 2, 3)
    attended = lax.map(one_group, (grouped, keys_all.transpose(1, 0, 2), values_all.transpose(1, 0, 2)))
    attended = attended.transpose(1, 0, 2, 3).reshape(slot_count, HEADS * HEAD_DIM).astype(jnp.bfloat16)
    head_delta = jnp.dot(attended, out_weight, preferred_element_type=jnp.float32)
    mixed_rows = raw_rows + head_delta
    second_square = lax.optimization_barrier(jnp.mean(mixed_rows * mixed_rows, axis=-1, keepdims=True))
    second_normed = (mixed_rows * lax.rsqrt(second_square + 1e-05) * mlp_gain.astype(jnp.float32)).astype(jnp.bfloat16)
    gate = jnp.dot(second_normed, gate_weight, preferred_element_type=jnp.float32)
    up_part = jnp.dot(second_normed, up_weight, preferred_element_type=jnp.float32)
    hidden = (jax.nn.silu(gate) * up_part).astype(jnp.bfloat16)
    mlp_delta = jnp.dot(hidden, down_weight, preferred_element_type=jnp.float32)
    update = (router_score[:, None] * (head_delta + mlp_delta)).astype(jnp.bfloat16)
    renewed = (raw_rows + update.astype(jnp.float32)).astype(jnp.bfloat16)
    return tokens.at[sources].set(renewed)
```

```python
import jax
import jax.numpy as jnp
from jax import lax
from jax.sharding import PartitionSpec as P


HEAD_DIM = 128
BF = jnp.bfloat16
F32 = jnp.float32
WIDTH = 256
GROUP = 4


def rotate(values, positions):
    half_dim = values.shape[-1] // 2
    exponent = jnp.arange(half_dim, dtype=F32) * (2.0 / values.shape[-1])
    frequency = 500000.0 ** (-exponent)
    angles = positions.astype(F32)[:, None] * frequency[None, :]
    cosine = jnp.cos(angles)
    sine_part = jnp.sin(angles)
    first_half = values[..., :half_dim]
    second_half = values[..., half_dim:]
    return jnp.concatenate(
        [
            first_half * cosine - second_half * sine_part,
            second_half * cosine + first_half * sine_part,
        ],
        axis=-1,
    )


def pick(array, index, axis):
    return lax.dynamic_index_in_dim(array, index, axis, keepdims=False)


class Grid:
    def __init__(self):
        self.C = lax.axis_size("ctx")
        self.M = lax.axis_size("mp")
        self.c = lax.axis_index("ctx")
        self.m = lax.axis_index("mp")
        self.H = self.C // self.M
        self.far_bits = []
        bit = 2
        while bit < self.C:
            self.far_bits.append(bit)
            bit *= 2

    def bit(self, b):
        return (self.c // b) % 2

    def swap(self, x, b):
        return lax.ppermute(x, "ctx", [(i, i ^ b) for i in range(self.C)])

    def flat(self, pairs):
        return [(a * self.M + b, d * self.M + e) for (a, b), (d, e) in pairs]

    def mp_sum(self, x):
        total = x
        for step in range(1, self.M):
            total = total + lax.ppermute(x, "mp", [(i, (i + step) % self.M) for i in range(self.M)])
        return total

    def far_gather(self, x, bits):
        have = []
        out = x[None]
        for b in bits:
            other = self.swap(out, b)
            zero = self.bit(b) == 0
            lo = jnp.where(zero, out, other)
            hi = jnp.where(zero, other, out)
            pos = sum(1 for g in have if g > b)
            lead = [2] * len(have)
            rest = x.shape
            lo = lo.reshape(*lead, *rest)
            hi = hi.reshape(*lead, *rest)
            out = jnp.stack([lo, hi], axis=pos)
            have.append(b)
            out = out.reshape(2 ** len(have), *rest)
        return out

    def gather(self, parts):
        a = self.far_gather(parts[0], self.far_bits)
        b = self.far_gather(parts[1], self.far_bits[::-1])
        near = jnp.concatenate([a, b], axis=-1)
        other = self.swap(near, 1)
        zero = self.bit(1) == 0
        lo = jnp.where(zero, near, other)
        hi = jnp.where(zero, other, near)
        out = jnp.stack([lo, hi], axis=1)
        return out.reshape(self.C, *near.shape[1:])

    def small_gather(self, x):
        out = self.far_gather(x, self.far_bits)
        other = self.swap(out, 1)
        zero = self.bit(1) == 0
        lo = jnp.where(zero, out, other)
        hi = jnp.where(zero, other, out)
        return jnp.stack([lo, hi], axis=1).reshape(self.C, *x.shape)

    def far_halve(self, x, bits):
        left = sorted(self.far_bits, reverse=True)
        rest = x.shape[1:]
        out = x
        for b in bits:
            pos = left.index(b)
            view = out.reshape(*([2] * len(left)), *rest)
            keep = pick(view, self.bit(b), pos)
            send = pick(view, 1 - self.bit(b), pos)
            left.remove(b)
            out = keep + self.swap(send.astype(BF), b).astype(F32)
        return out.reshape(rest)

    def near_halve(self, x):
        view = x.reshape(self.C // 2, 2, *x.shape[1:])
        keep = pick(view, self.bit(1), 1)
        send = pick(view, 1 - self.bit(1), 1)
        return keep + self.swap(send.astype(BF), 1).astype(F32)

    def scatter_sum(self, x):
        near = self.near_halve(x)
        half = x.shape[-1] // 2
        a = self.far_halve(near[..., :half], self.far_bits[::-1])
        b = self.far_halve(near[..., half:], self.far_bits)
        return jnp.concatenate([a, b], axis=-1)

    def rows_to_slices(self, local_rows):
        n = local_rows.shape[0]
        f = local_rows.shape[1] // self.H
        payload = [
            lax.dynamic_slice(local_rows, (0, ((self.c % self.H) ^ i) * f), (n, f))
            for i in range(self.H)
        ]
        q = self.c % self.H + self.H * self.m
        out = jnp.zeros((self.C * n, f), local_rows.dtype)
        for r in range(self.C):
            pairs = [
                ((a, b), (self.H * b + (a ^ r) % self.H, (a ^ r) // self.H))
                for a in range(self.C)
                for b in range(self.M)
            ]
            got = lax.ppermute(payload[r % self.H], ("ctx", "mp"), self.flat(pairs))
            out = lax.dynamic_update_slice(out, got, ((q ^ r) * n, 0))
        return out

    def slices_to_rows(self, partial):
        n = partial.shape[0] // self.C
        f = partial.shape[1]
        half = partial.astype(BF)
        q = self.c % self.H + self.H * self.m
        sums = [None] * self.H
        for r in range(self.C):
            pairs = [
                ((self.H * b + (a ^ r) % self.H, (a ^ r) // self.H), (a, b))
                for a in range(self.C)
                for b in range(self.M)
            ]
            block = lax.dynamic_slice(half, ((q ^ r) * n, 0), (n, f))
            got = lax.ppermute(block, ("ctx", "mp"), self.flat(pairs)).astype(F32)
            i = r % self.H
            sums[i] = got if sums[i] is None else sums[i] + got
        out = jnp.zeros((n, self.H * f), F32)
        for i in range(self.H):
            out = lax.dynamic_update_slice(out, sums[i], (0, ((self.c % self.H) ^ i) * f))
        return out


def head_reduce(grid, partial, rows, q_local, kv_local):
    heads = partial.reshape(rows, q_local + 2 * kv_local, HEAD_DIM).transpose(1, 0, 2)
    group_span = grid.C // kv_local
    queries = grid.near_halve(heads[:q_local])
    pair = heads[q_local:].reshape(2, kv_local, rows, HEAD_DIM)
    keep = pick(pair, grid.bit(1), 0)
    send = pick(pair, 1 - grid.bit(1), 0)
    stored = keep + grid.swap(send.astype(BF), 1).astype(F32)
    half = rows // 2
    halves = []
    for span, order in ((slice(0, half), grid.far_bits[::-1]), (slice(half, rows), grid.far_bits)):
        q = queries[:, span]
        kv = stored[:, span]
        left = sorted(grid.far_bits, reverse=True)
        left_kv = [b for b in left if b >= group_span]
        for b in order:
            view = q.reshape(*([2] * len(left)), half, HEAD_DIM)
            pos = left.index(b)
            q_keep = pick(view, grid.bit(b), pos)
            q_send = pick(view, 1 - grid.bit(b), pos).reshape(-1, half, HEAD_DIM)
            left.remove(b)
            if b >= group_span:
                kv_view = kv.reshape(*([2] * len(left_kv)), half, HEAD_DIM)
                kv_pos = left_kv.index(b)
                kv_keep = pick(kv_view, grid.bit(b), kv_pos).reshape(-1, half, HEAD_DIM)
                kv_send = pick(kv_view, 1 - grid.bit(b), kv_pos).reshape(-1, half, HEAD_DIM)
                left_kv.remove(b)
            else:
                kv_keep = kv
                kv_send = kv
            got = grid.swap(jnp.concatenate([q_send, kv_send], axis=0).astype(BF), b).astype(F32)
            count = q_send.shape[0]
            q = q_keep.reshape(-1, half, HEAD_DIM) + got[:count]
            kv = kv_keep + got[count:]
        halves.append((q.reshape(half, HEAD_DIM), kv.reshape(half, HEAD_DIM)))
    query = jnp.concatenate([halves[0][0], halves[1][0]], axis=0)
    own = jnp.concatenate([halves[0][1], halves[1][1]], axis=0)
    return query, own


def feed_forward(grid, normed, gate_weight, up_weight, down_weight):
    C, M = grid.C, grid.M
    rows = normed.shape[0]
    hidden_cols = gate_weight.shape[1]
    width = WIDTH if hidden_cols % WIDTH == 0 else HEAD_DIM
    count = hidden_cols // width
    streams = 2
    place = jnp.where(grid.c % 2 == 1, grid.m, M - 1 - grid.m)

    def at(a, p):
        return (a, p if a % 2 == 1 else M - 1 - p)

    inward = grid.flat([(at(a, p), at(a, p + 1)) for a in range(C) for p in range(M - 1)])
    outward = grid.flat([(at(a, p + 1), at(a, p)) for a in range(C) for p in range(M - 1)])

    def choose(options):
        return lax.select_n(place, *options)

    partial = {}

    def part(k):
        if k not in partial:
            lo, hi = k * width, (k + 1) * width
            g = jnp.dot(normed, gate_weight[:, lo:hi], preferred_element_type=F32)
            u = jnp.dot(normed, up_weight[:, lo:hi], preferred_element_type=F32)
            partial[k] = jnp.concatenate([g.astype(BF), u.astype(BF)], axis=1)
        return partial[k]

    lists = [list(range(s, count, streams)) for s in range(streams)]
    got = [None] * streams
    passed = [None] * streams
    hist = [[] for _ in range(streams)]
    hids = [[] for _ in range(streams)]
    waiting = []
    total = None
    zero = jnp.zeros((rows, 2 * width), BF)
    tick = normed[:8, :128].astype(F32) * 0.0
    last = max(len(ks) for ks in lists) + 2 * (M - 1) - 1
    for t in range(last + 1):
        for s in range(streams):
            ks = lists[s]
            n = len(ks)
            came = got[s]
            if t < n + M - 2:
                options = [part(ks[t - p]) if 0 <= t - p < n else zero for p in range(M - 1)]
                own = choose(options + [zero])
                send = own if came is None else (own.astype(F32) + came.astype(F32)).astype(BF)
                got[s] = lax.ppermute(send, ("ctx", "mp"), inward)
            i = t - (M - 1)
            if 0 <= i < n + M - 2:
                if i < n:
                    full = came.astype(F32) + part(ks[i]).astype(F32)
                    g, u = full[:, :width], full[:, width:]
                    hids[s].append((jax.nn.silu(g) * u).astype(BF))
                fresh = hids[s][i] if i < n else jnp.zeros((rows, width), BF)
                send = fresh if passed[s] is None else jnp.where(place == M - 1, fresh, passed[s])
                passed[s] = lax.ppermute(send, ("ctx", "mp"), outward)
                hist[s].append(passed[s])
            j = i - (M - 2) - 1
            if 0 <= j < n:
                waiting.append(
                    (ks[j], choose([hist[s][j + M - 2 - p] for p in range(M - 1)] + [hids[s][j]]))
                )
            tick = tick * 0.5
            tick = lax.optimization_barrier(tick)
            final = t == last and s == streams - 1
            if len(waiting) >= GROUP or (final and waiting):
                waiting.sort(key=lambda kv: kv[0])
                k0, k1 = waiting[0][0], waiting[-1][0] + 1
                assert k1 - k0 == len(waiting)
                block = lax.optimization_barrier(jnp.concatenate([b for _, b in waiting], axis=1))
                waiting.clear()
                piece = jnp.dot(
                    block, down_weight[k0 * width : k1 * width], preferred_element_type=F32
                )
                total = lax.optimization_barrier(piece if total is None else total + piece)
    return total, jnp.sum(tick)


def body(
    tokens,
    norm_gain,
    router_weight,
    query_weight,
    key_weight,
    value_weight,
    out_weight,
    mlp_gain,
    gate_weight,
    up_weight,
    down_weight,
    destination,
    kept_pos,
):
    grid = Grid()
    ctx_count, mp_count = grid.C, grid.M
    my_index = grid.c
    tok_dev = tokens.shape[0]
    kept_dev = kept_pos.shape[0]
    rows = kept_dev * ctx_count
    feature_cols = tokens.shape[1]
    feature_total = feature_cols * mp_count
    slice_cols = feature_total // ctx_count
    capacity = (3 * kept_dev // 2 + ctx_count - 1) // ctx_count
    slots_all = ctx_count * capacity
    head_dim = HEAD_DIM
    query_cols = query_weight.shape[1]
    key_cols = key_weight.shape[1]
    kv_local = key_cols // head_dim
    q_local = query_cols // head_dim
    group_size = q_local // kv_local
    peer_ids = jnp.arange(ctx_count, dtype=jnp.int32)
    is_kept = destination >= 0
    owner_ids = destination // kept_dev
    slot_ids = destination % kept_dev
    kept_order = slot_ids * ctx_count + owner_ids
    first_order = jnp.min(jnp.where(is_kept, kept_order, ctx_count * kept_dev))
    first_slots = (first_order - peer_ids + ctx_count - 1) // ctx_count
    owner_match = owner_ids[:, None] == peer_ids[None, :]
    send_index = (
        owner_ids * capacity
        + slot_ids
        - jnp.sum(jnp.where(owner_match, first_slots[None, :], 0), axis=1)
    )
    send_index = jnp.where(is_kept, send_index, slots_all)
    token_ids = jnp.arange(tok_dev, dtype=jnp.int32)
    picked = jnp.full((slots_all,), tok_dev, jnp.int32).at[send_index].set(token_ids, mode="drop")
    outgoing = jnp.take(tokens, picked, axis=0, mode="fill", fill_value=0).reshape(
        ctx_count, capacity, feature_cols
    )
    incoming = lax.all_to_all(outgoing, "ctx", split_axis=0, concat_axis=0, tiled=True).reshape(
        slots_all, feature_cols
    )
    slot_range = jnp.arange(kept_dev, dtype=jnp.int32)
    source_ids = kept_pos // tok_dev
    source_match = source_ids[:, None] == peer_ids[None, :]
    first_from = jnp.min(jnp.where(source_match, slot_range[:, None], kept_dev), axis=0)
    recv_index = (
        source_ids * capacity
        + slot_range
        - jnp.sum(jnp.where(source_match, first_from[None, :], 0), axis=1)
    )
    local_rows = incoming[recv_index]
    raw_share = local_rows.astype(F32)
    slices = grid.rows_to_slices(local_rows)
    my_router = lax.dynamic_slice(router_weight, (grid.m * feature_cols,), (feature_cols,))
    sums = grid.mp_sum(
        jnp.stack(
            [
                jnp.sum(raw_share * raw_share, axis=1),
                jnp.sum(raw_share * my_router.astype(F32)[None, :], axis=1),
            ]
        )
    )
    router_score = jax.nn.sigmoid(sums[1])
    inverse = lax.rsqrt(sums[0] / feature_total + 1e-05)
    shared = grid.small_gather(jnp.stack([inverse, kept_pos.astype(F32)]))
    inverse_all = shared[:, 0].reshape(rows)
    pos_all = shared[:, 1].reshape(rows)
    my_gain = lax.dynamic_slice(norm_gain, (my_index * slice_cols,), (slice_cols,))
    scaled = (slices.astype(F32) * my_gain.astype(F32)[None, :]).astype(BF)
    stacked = jnp.concatenate([query_weight, key_weight, value_weight], axis=1)
    projected = jnp.dot(scaled, stacked, preferred_element_type=F32)
    row_ids = jnp.arange(rows, dtype=jnp.int32)
    row_order = row_ids % kept_dev * ctx_count + row_ids // kept_dev
    softmax_scale = head_dim ** (-0.5)
    if q_local == ctx_count and kv_local <= ctx_count // 2:
        query, own = head_reduce(grid, projected, rows, q_local, kv_local)
        query = rotate(query * inverse_all[:, None], pos_all).astype(BF)
        own = own * inverse_all[:, None]
        own = jnp.where(grid.bit(1) == 0, rotate(own, pos_all), own).astype(BF)
        other = grid.swap(own, 1)
        keys = jnp.where(grid.bit(1) == 0, own, other)
        values = jnp.where(grid.bit(1) == 0, other, own)
        allowed = row_order[None, :] <= row_order[:, None]
        scores = (
            lax.dot_general(query, keys, (((1,), (1,)), ((), ())), preferred_element_type=F32)
            * softmax_scale
        )
        scores = jnp.where(allowed, scores, -1e30)
        peak = jnp.max(scores, axis=-1, keepdims=True)
        weights = jnp.where(allowed, jnp.exp(scores - peak), 0.0)
        weighted = jnp.dot(weights, values.astype(F32))
        attended = (weighted / jnp.sum(weights, axis=-1, keepdims=True)).astype(BF)
        half = rows // 2
        first = grid.far_gather(attended[:half], grid.far_bits)
        second = grid.far_gather(attended[half:], grid.far_bits[::-1])
        near = jnp.concatenate([first, second], axis=1)
        other = grid.swap(near, 1)
        zero = grid.bit(1) == 0
        pair = jnp.stack([jnp.where(zero, near, other), jnp.where(zero, other, near)], axis=1)
        every_head = pair.reshape(q_local, rows, head_dim).transpose(1, 0, 2).reshape(rows, query_cols)
    else:
        mine = lax.psum_scatter(projected, "ctx", scatter_dimension=0, tiled=True)
        mine = mine * inverse[:, None]
        by_head = mine.reshape(kept_dev, q_local + 2 * kv_local, head_dim).transpose(1, 0, 2)
        queries = rotate(by_head[:q_local], kept_pos).astype(BF)
        queries = queries.reshape(kv_local, group_size, kept_dev, head_dim)
        keys = rotate(by_head[q_local : q_local + kv_local], kept_pos).astype(BF)
        values = by_head[q_local + kv_local :].astype(BF)
        keys = lax.all_gather(keys, "ctx", axis=1, tiled=True)
        values = lax.all_gather(values, "ctx", axis=1, tiled=True)
        query_order = slot_range * ctx_count + my_index
        allowed = row_order[None, :] <= query_order[:, None]
        scores = (
            jnp.einsum("hgqd,hkd->hgqk", queries, keys, preferred_element_type=F32) * softmax_scale
        )
        scores = jnp.where(allowed, scores, -1e30)
        peak = jnp.max(scores, axis=-1, keepdims=True)
        weights = jnp.where(allowed, jnp.exp(scores - peak), 0.0)
        weighted = jnp.einsum("hgqk,hkd->hgqd", weights, values.astype(F32))
        attended = weighted / jnp.sum(weights, axis=-1, keepdims=True)
        attended = attended.transpose(2, 0, 1, 3).reshape(kept_dev, query_cols).astype(BF)
        every_head = lax.all_gather(attended, "ctx", axis=0, tiled=True)
    partial_cols = jnp.dot(every_head, out_weight, preferred_element_type=F32)
    head_share = grid.slices_to_rows(partial_cols)
    mixed_share = raw_share + head_share
    square_sum = grid.mp_sum(jnp.sum(mixed_share * mixed_share, axis=1).reshape(1, kept_dev))[0]
    second_normed = (
        mixed_share
        * lax.rsqrt(square_sum / feature_total + 1e-05)[:, None]
        * mlp_gain.astype(F32)
    ).astype(BF)
    mid = feature_cols // 2
    every_normed = grid.gather((second_normed[:, :mid], second_normed[:, mid:]))
    every_normed = every_normed.reshape(rows, feature_cols)
    mlp_partial, tick = feed_forward(grid, every_normed, gate_weight, up_weight, down_weight)
    mlp_share = grid.scatter_sum(mlp_partial.reshape(ctx_count, kept_dev, feature_cols))
    update = (router_score[:, None] * (head_share + mlp_share) + tick).astype(BF)
    returning = (
        jnp.zeros((slots_all, feature_cols), BF)
        .at[recv_index]
        .set(update)
        .reshape(ctx_count, capacity, feature_cols)
    )
    returned = lax.all_to_all(returning, "ctx", split_axis=0, concat_axis=0, tiled=True).reshape(
        slots_all, feature_cols
    )
    arriving = jnp.take(returned, send_index, axis=0, mode="fill", fill_value=0)
    return (tokens.astype(F32) + arriving.astype(F32)).astype(BF)


def solution(mesh):
    in_specs = (
        P("ctx", "mp"),
        P(),
        P(),
        P("ctx", "mp"),
        P("ctx", "mp"),
        P("ctx", "mp"),
        P("mp", "ctx"),
        P("mp"),
        P("mp", "ctx"),
        P("mp", "ctx"),
        P("ctx", "mp"),
        P("ctx"),
        P("ctx"),
    )
    out_specs = P("ctx", "mp")
    return jax.shard_map(body, mesh=mesh, in_specs=in_specs, out_specs=out_specs, check_vma=False)
```

```python
import jax
import jax.numpy as jnp
from jax import lax
from jax.sharding import PartitionSpec as P


HEAD_DIM = 128
BF = jnp.bfloat16
F32 = jnp.float32
WIDTH = 256
EARLY = 10


def rotate(values, positions):
    half_dim = values.shape[-1] // 2
    exponent = jnp.arange(half_dim, dtype=F32) * (2.0 / values.shape[-1])
    frequency = 500000.0 ** (-exponent)
    angles = positions.astype(F32)[:, None] * frequency[None, :]
    cosine = jnp.cos(angles)
    sine_part = jnp.sin(angles)
    first_half = values[..., :half_dim]
    second_half = values[..., half_dim:]
    return jnp.concatenate(
        [
            first_half * cosine - second_half * sine_part,
            second_half * cosine + first_half * sine_part,
        ],
        axis=-1,
    )


def flip_blocks(x, b):
    view = x.reshape(x.shape[0] // (2 * b), 2, b, *x.shape[1:])
    return view[:, ::-1].reshape(x.shape)


class Grid:
    def __init__(self):
        self.C = lax.axis_size("ctx")
        self.M = lax.axis_size("mp")
        self.c = lax.axis_index("ctx")
        self.m = lax.axis_index("mp")
        self.H = self.C // self.M
        self.far_bits = []
        bit = 2
        while bit < self.C:
            self.far_bits.append(bit)
            bit *= 2
        self.even = list(range(0, self.C, 2))
        self.order = self.even + [i + 1 for i in self.even]

    def bit(self, b):
        return (self.c // b) % 2

    def swap(self, x, b):
        return lax.ppermute(x, "ctx", [(i, i ^ b) for i in range(self.C)])

    def flat(self, pairs):
        return [(a * self.M + b, d * self.M + e) for (a, b), (d, e) in pairs]

    def rotate_mp(self, block_for):
        return [
            lax.ppermute(block_for(s), "mp", [(i, (i + s) % self.M) for i in range(self.M)])
            for s in range(1, self.M)
        ]

    def mp_sum(self, x):
        total = x
        for other in self.rotate_mp(lambda s: x):
            total = total + other
        return total

    def far_gather(self, x, bits):
        have = {0: x}
        for b in bits:
            keys = list(have)
            got = self.swap(jnp.stack([have[k] for k in keys]), b)
            for j, k in enumerate(keys):
                have[k ^ b] = got[j]
        return have

    def gather(self, parts):
        a = self.far_gather(parts[0], self.far_bits)
        b = self.far_gather(parts[1], self.far_bits[::-1])
        near = jnp.concatenate(
            [jnp.concatenate([a[i], b[i]], axis=1) for i in self.even], axis=0
        )
        return jnp.concatenate([near, self.swap(near, 1)], axis=0)

    def small_gather(self, x):
        near = self.far_gather(x, self.far_bits)
        near = jnp.stack([near[i] for i in self.even])
        other = self.swap(near, 1)
        return jnp.stack([near, other], axis=1).reshape(self.C, *x.shape)

    def xor_order(self, x, value):
        b = 1
        while b < self.C:
            x = jnp.where((value // b) % 2 == 1, flip_blocks(x, b), x)
            b *= 2
        return x

    def far_halve(self, blocks, bits):
        for b in bits:
            keep = [k for k in blocks if not k & b]
            got = self.swap(jnp.stack([blocks[k ^ b] for k in keep]).astype(BF), b)
            blocks = {k: blocks[k] + got[j].astype(F32) for j, k in enumerate(keep)}
        return blocks[0]

    def scatter_sum(self, near, far):
        half = near.shape[1] // 2
        n = near.shape[0] // len(self.even)
        near = near + self.swap(far.astype(BF), 1).astype(F32)
        parts = []
        for cols, bits in (
            (slice(0, half), self.far_bits[::-1]),
            (slice(half, None), self.far_bits),
        ):
            blocks = {i: near[j * n : (j + 1) * n, cols] for j, i in enumerate(self.even)}
            parts.append(self.far_halve(blocks, bits))
        return jnp.concatenate(parts, axis=1)

    def rows_to_slices(self, local_rows):
        n = local_rows.shape[0]
        f = local_rows.shape[1] // self.H
        payload = [
            lax.dynamic_slice(local_rows, (0, ((self.c % self.H) ^ i) * f), (n, f))
            for i in range(self.H)
        ]
        blocks = []
        for r in range(self.C):
            pairs = [
                ((a, b), (self.H * b + (a ^ r) % self.H, (a ^ r) // self.H))
                for a in range(self.C)
                for b in range(self.M)
            ]
            blocks.append(lax.ppermute(payload[r % self.H], ("ctx", "mp"), self.flat(pairs)))
        arrived = blocks[1]
        b = 1
        while b < self.H:
            swapped = self.bit(b) == 1
            blocks = [jnp.where(swapped, blocks[r ^ b], blocks[r]) for r in range(self.C)]
            b *= 2
        return blocks, arrived

    def slices_to_rows(self, partial):
        n = partial.shape[0] // self.C
        f = partial.shape[1]
        first = self.H * self.m
        full = jnp.zeros((self.C, n, f), BF)
        for r in range(self.C):
            got = lax.dynamic_slice(partial, (((self.c ^ r) ^ first) * n, 0), (n, f))
            if r:
                got = self.swap(got, r)
            full = lax.dynamic_update_slice(full, got[None], (self.c ^ r, 0, 0))

        def share(s):
            return lax.dynamic_slice(full, ((self.m + s) % self.M * self.H, 0, 0), (self.H, n, f))

        total = share(0).astype(F32)
        for got in self.rotate_mp(share):
            total = total + got.astype(F32)
        return [total[h] for h in range(self.H)]


def columns(weight, index):
    return lax.dynamic_slice(
        weight, (0, index * HEAD_DIM), (weight.shape[0], HEAD_DIM)
    )


def head_weights(grid, query_weight, key_weight, value_weight):
    group = grid.c // (grid.C // 2)
    odd = grid.bit(1) == 1
    mine = jnp.where(odd, value_weight, key_weight)
    other = jnp.where(odd, key_weight, value_weight)

    def side(near, kv):
        parts = []
        for g in range(2):
            parts += [columns(query_weight, grid.c ^ (i + near)) for i in grid.even[2 * g : 2 * g + 2]]
            parts.append(columns(kv, group ^ g))
        return jnp.concatenate(parts, axis=1)

    return side(1, other), side(0, mine)


def head_reduce(grid, send, keep):
    d = HEAD_DIM
    near = keep + grid.swap(send, 1).astype(F32)
    half = near.shape[0] // 2
    group_bit = grid.C // 2
    side_bit = grid.far_bits[0]
    first, second = near[:half], near[half:]
    got = grid.swap(first[:, 3 * d :].astype(BF), group_bit).astype(F32)
    a = first[:, : 3 * d] + got
    out = jnp.concatenate([second[:, d : 3 * d], second[:, 4 * d :]], axis=1).astype(BF)
    got = grid.swap(out, side_bit).astype(F32)
    b0 = second[:, :d] + got[:, :d]
    bg0 = second[:, 2 * d : 3 * d] + got[:, d : 2 * d]
    b4 = second[:, 3 * d : 4 * d] + got[:, 2 * d : 3 * d]
    bg1 = second[:, 5 * d :] + got[:, 3 * d :]
    got = grid.swap(a[:, d:].astype(BF), side_bit).astype(F32)
    query_a = a[:, :d] + got[:, :d]
    own_a = a[:, 2 * d :] + got[:, d:]
    got = grid.swap(jnp.concatenate([b4, bg1], axis=1).astype(BF), group_bit).astype(F32)
    query_b = b0 + got[:, :d]
    own_b = bg0 + got[:, d:]
    return jnp.concatenate([query_a, query_b], axis=0), jnp.concatenate([own_a, own_b], axis=0)


def feed_forward(grid, normed, scale, gate_weight, up_weight, down_weight):
    C, M = grid.C, grid.M
    rows = normed.shape[0]
    hidden_cols = gate_weight.shape[1]
    width = WIDTH if hidden_cols % WIDTH == 0 else HEAD_DIM
    count = hidden_cols // width
    streams = 2
    place = jnp.where(grid.c % 2 == 1, grid.m, M - 1 - grid.m)

    def at(a, p):
        return (a, p if a % 2 == 1 else M - 1 - p)

    inward = grid.flat([(at(a, p), at(a, p + 1)) for a in range(C) for p in range(M - 1)])
    outward = grid.flat([(at(a, p + 1), at(a, p)) for a in range(C) for p in range(M - 1)])

    def choose(options):
        return lax.select_n(place, *options)

    partial = {}

    def part(k):
        if k not in partial:
            lo, hi = k * width, (k + 1) * width
            g = jnp.dot(normed, gate_weight[:, lo:hi], preferred_element_type=F32)
            u = jnp.dot(normed, up_weight[:, lo:hi], preferred_element_type=F32)
            partial[k] = jnp.concatenate([g.astype(BF), u.astype(BF)], axis=1)
        return partial[k]

    lists = [list(range(s, count, streams)) for s in range(streams)]
    got = [None] * streams
    passed = [None] * streams
    hist = [[] for _ in range(streams)]
    hids = [[] for _ in range(streams)]
    waiting = []
    taken = 0
    total = None
    zero = jnp.zeros((rows, 2 * width), BF)
    tick = normed[:8, :128].astype(F32) * 0.0
    last = max(len(ks) for ks in lists) + 2 * (M - 1) - 1
    for t in range(last + 1):
        for s in range(streams):
            ks = lists[s]
            n = len(ks)
            came = got[s]
            if t < n + M - 2:
                options = [part(ks[t - p]) if 0 <= t - p < n else zero for p in range(M - 1)]
                own = choose(options + [zero])
                send = own if came is None else (own.astype(F32) + came.astype(F32)).astype(BF)
                got[s] = lax.ppermute(send, ("ctx", "mp"), inward)
            i = t - (M - 1)
            if 0 <= i < n + M - 2:
                if i < n:
                    full = came.astype(F32) + part(ks[i]).astype(F32)
                    g, u = full[:, :width] * scale, full[:, width:] * scale
                    hids[s].append((jax.nn.silu(g) * u).astype(BF))
                fresh = hids[s][i] if i < n else jnp.zeros((rows, width), BF)
                send = fresh if passed[s] is None else jnp.where(place == M - 1, fresh, passed[s])
                passed[s] = lax.ppermute(send, ("ctx", "mp"), outward)
                hist[s].append(passed[s])
            j = i - (M - 2) - 1
            if 0 <= j < n:
                options = [hist[s][j + M - 2 - p] for p in range(M - 1)] + [hids[s][j]]
                here = place
                if taken:
                    *options, here = lax.optimization_barrier((*options, place))
                waiting.append((ks[j], lax.select_n(here, *options)))
            tick = tick * 0.5
            tick = lax.optimization_barrier(tick)
            final = t == last and s == streams - 1
            if (not taken and len(waiting) >= EARLY) or (final and waiting):
                waiting.sort(key=lambda kv: kv[0])
                k0, k1 = waiting[0][0], waiting[-1][0] + 1
                assert k1 - k0 == len(waiting)
                block = lax.optimization_barrier(jnp.concatenate([b for _, b in waiting], axis=1))
                taken += len(waiting)
                waiting.clear()
                weight = down_weight[k0 * width : k1 * width]
                if final:
                    half = rows // 2
                    far = jnp.dot(block[half:], weight, preferred_element_type=F32)
                    near = jnp.dot(block[:half], weight, preferred_element_type=F32)
                    if total is not None:
                        far = far + total[half:]
                        near = near + total[:half]
                    total = near, far
                else:
                    total = jnp.dot(block, weight, preferred_element_type=F32)
                    total = lax.optimization_barrier(total)
    return *total, jnp.sum(tick)


def body(
    tokens,
    norm_gain,
    router_weight,
    query_weight,
    key_weight,
    value_weight,
    out_weight,
    mlp_gain,
    gate_weight,
    up_weight,
    down_weight,
    destination,
    kept_pos,
):
    grid = Grid()
    ctx_count, mp_count = grid.C, grid.M
    my_index = grid.c
    tok_dev = tokens.shape[0]
    kept_dev = kept_pos.shape[0]
    rows = kept_dev * ctx_count
    feature_cols = tokens.shape[1]
    feature_total = feature_cols * mp_count
    slice_cols = feature_total // ctx_count
    capacity = (3 * kept_dev // 2 + ctx_count - 1) // ctx_count
    slots_all = ctx_count * capacity
    head_dim = HEAD_DIM
    query_cols = query_weight.shape[1]
    key_cols = key_weight.shape[1]
    kv_local = key_cols // head_dim
    q_local = query_cols // head_dim
    group_size = q_local // kv_local
    peer_ids = jnp.arange(ctx_count, dtype=jnp.int32)
    is_kept = destination >= 0
    owner_ids = destination // kept_dev
    slot_ids = destination % kept_dev
    kept_order = slot_ids * ctx_count + owner_ids
    first_order = jnp.min(jnp.where(is_kept, kept_order, ctx_count * kept_dev))
    first_slots = (first_order - peer_ids + ctx_count - 1) // ctx_count
    owner_match = owner_ids[:, None] == peer_ids[None, :]
    send_index = (
        owner_ids * capacity
        + slot_ids
        - jnp.sum(jnp.where(owner_match, first_slots[None, :], 0), axis=1)
    )
    send_index = jnp.where(is_kept, send_index, slots_all)
    slot_ids_all = jnp.arange(slots_all, dtype=jnp.int32)
    takes = (slot_ids_all[:, None] == send_index[None, :]).astype(BF)
    outgoing = (
        jnp.dot(takes, tokens, preferred_element_type=F32)
        .astype(BF)
        .reshape(ctx_count, capacity, feature_cols)
    )
    incoming = lax.all_to_all(outgoing, "ctx", split_axis=0, concat_axis=0, tiled=True).reshape(
        slots_all, feature_cols
    )
    slot_range = jnp.arange(kept_dev, dtype=jnp.int32)
    source_ids = kept_pos // tok_dev
    source_match = source_ids[:, None] == peer_ids[None, :]
    first_from = jnp.min(jnp.where(source_match, slot_range[:, None], kept_dev), axis=0)
    recv_index = (
        source_ids * capacity
        + slot_range
        - jnp.sum(jnp.where(source_match, first_from[None, :], 0), axis=1)
    )
    local_rows = incoming[recv_index]
    fits = q_local == ctx_count and kv_local == 2 and len(grid.far_bits) == 2
    blocks, arrived = grid.rows_to_slices(local_rows)
    my_rows, _ = lax.optimization_barrier((local_rows, arrived))
    raw_share = my_rows.astype(F32)
    my_router = lax.dynamic_slice(router_weight, (grid.m * feature_cols,), (feature_cols,))
    sums = grid.mp_sum(
        jnp.stack(
            [
                jnp.sum(raw_share * raw_share, axis=1),
                jnp.sum(raw_share * my_router.astype(F32)[None, :], axis=1),
            ]
        )
    )
    router_score = jax.nn.sigmoid(sums[1])
    inverse = lax.rsqrt(sums[0] / feature_total + 1e-05)
    shared = grid.small_gather(jnp.stack([inverse, kept_pos.astype(F32)]))
    shared = grid.xor_order(shared, my_index ^ (grid.H * grid.m))
    inverse_all = shared[:, 0].reshape(rows)
    pos_all = shared[:, 1].reshape(rows)
    my_gain = lax.dynamic_slice(norm_gain, (my_index * slice_cols,), (slice_cols,))
    my_gain = my_gain.astype(F32)[None, :]
    scaled = jnp.concatenate([(b.astype(F32) * my_gain).astype(BF) for b in blocks], axis=0)
    softmax_scale = head_dim ** (-0.5)
    if fits:
        send_weight, keep_weight = head_weights(grid, query_weight, key_weight, value_weight)
        out_rows = jnp.concatenate(
            [
                lax.dynamic_slice(
                    out_weight, ((my_index ^ i) * head_dim, 0), (head_dim, out_weight.shape[1])
                )
                for i in grid.order
            ],
            axis=0,
        )
        send = jnp.dot(scaled, send_weight, preferred_element_type=F32).astype(BF)
        keep = jnp.dot(scaled, keep_weight, preferred_element_type=F32)
        query, own = head_reduce(grid, send, keep)
        query = rotate(query * inverse_all[:, None], pos_all).astype(BF)
        own = own * inverse_all[:, None]
        even = grid.bit(1) == 0
        own = jnp.where(even, rotate(own, pos_all), own).astype(BF)
        other = grid.swap(own, 1)
        keys = jnp.where(even, own, other)
        values = jnp.where(even, other, own)
        allowed = pos_all[None, :] <= pos_all[:, None]
        scores = (
            lax.dot_general(query, keys, (((1,), (1,)), ((), ())), preferred_element_type=F32)
            * softmax_scale
        )
        scores = jnp.where(allowed, scores, -1e30)
        peak = jnp.max(scores, axis=-1, keepdims=True)
        weights = jnp.where(allowed, jnp.exp(scores - peak), 0.0)
        weighted = jnp.dot(weights, values.astype(F32))
        attended = (weighted / jnp.sum(weights, axis=-1, keepdims=True)).astype(BF)
        half = rows // 2
        first = grid.far_gather(attended[:half], grid.far_bits)
        second = grid.far_gather(attended[half:], grid.far_bits[::-1])
        near = jnp.concatenate(
            [jnp.concatenate([first[i], second[i]], axis=0) for i in grid.even], axis=1
        )
        span = len(grid.even) * head_dim
        partial_cols = jnp.dot(near, out_rows[:span], preferred_element_type=F32) + jnp.dot(
            grid.swap(near, 1), out_rows[span:], preferred_element_type=F32
        )
    else:
        stacked = jnp.concatenate([query_weight, key_weight, value_weight], axis=1)
        projected = jnp.dot(scaled, stacked, preferred_element_type=F32)
        mine = lax.psum_scatter(projected, "ctx", scatter_dimension=0, tiled=True)
        my_inverse = lax.dynamic_slice(inverse_all, (my_index * kept_dev,), (kept_dev,))
        my_pos = lax.dynamic_slice(pos_all, (my_index * kept_dev,), (kept_dev,))
        mine = mine * my_inverse[:, None]
        by_head = mine.reshape(kept_dev, q_local + 2 * kv_local, head_dim).transpose(1, 0, 2)
        queries = rotate(by_head[:q_local], my_pos).astype(BF)
        queries = queries.reshape(kv_local, group_size, kept_dev, head_dim)
        keys = rotate(by_head[q_local : q_local + kv_local], my_pos).astype(BF)
        values = by_head[q_local + kv_local :].astype(BF)
        keys = lax.all_gather(keys, "ctx", axis=1, tiled=True)
        values = lax.all_gather(values, "ctx", axis=1, tiled=True)
        allowed = pos_all[None, :] <= my_pos[:, None]
        scores = (
            jnp.einsum("hgqd,hkd->hgqk", queries, keys, preferred_element_type=F32) * softmax_scale
        )
        scores = jnp.where(allowed, scores, -1e30)
        peak = jnp.max(scores, axis=-1, keepdims=True)
        weights = jnp.where(allowed, jnp.exp(scores - peak), 0.0)
        weighted = jnp.einsum("hgqk,hkd->hgqd", weights, values.astype(F32))
        attended = weighted / jnp.sum(weights, axis=-1, keepdims=True)
        attended = attended.transpose(2, 0, 1, 3).reshape(kept_dev, query_cols).astype(BF)
        every_head = lax.all_gather(attended, "ctx", axis=0, tiled=True)
        partial_cols = jnp.dot(every_head, out_weight, preferred_element_type=F32)
    head_share = jnp.concatenate(grid.slices_to_rows(partial_cols.astype(BF)), axis=1)
    mixed_share = raw_share + head_share
    square_sum = grid.mp_sum(jnp.sum(mixed_share * mixed_share, axis=1))
    second_inverse = grid.small_gather(lax.rsqrt(square_sum / feature_total + 1e-05))
    second_inverse = second_inverse[jnp.array(grid.order)].reshape(rows, 1)
    second_scaled = (mixed_share * mlp_gain.astype(F32)).astype(BF)
    mid = feature_cols // 2
    every_scaled = grid.gather((second_scaled[:, :mid], second_scaled[:, mid:]))
    near, far, tick = feed_forward(
        grid, every_scaled, second_inverse, gate_weight, up_weight, down_weight
    )
    mlp_share = grid.scatter_sum(near, far)
    update = (router_score[:, None] * (head_share + mlp_share) + tick).astype(BF)
    places = (slot_ids_all[:, None] == recv_index[None, :]).astype(BF)
    returning = (
        jnp.dot(places, update, preferred_element_type=F32)
        .astype(BF)
        .reshape(ctx_count, capacity, feature_cols)
    )
    returned = lax.all_to_all(returning, "ctx", split_axis=0, concat_axis=0, tiled=True).reshape(
        slots_all, feature_cols
    )
    lands = (send_index[:, None] == slot_ids_all[None, :]).astype(BF)
    arriving = jnp.dot(lands, returned, preferred_element_type=F32)
    return (tokens.astype(F32) + arriving).astype(BF)


def solution(mesh):
    in_specs = (
        P("ctx", "mp"),
        P(),
        P(),
        P("ctx", "mp"),
        P("ctx", "mp"),
        P("ctx", "mp"),
        P("mp", "ctx"),
        P("mp"),
        P("mp", "ctx"),
        P("mp", "ctx"),
        P("ctx", "mp"),
        P("ctx"),
        P("ctx"),
    )
    out_specs = P("ctx", "mp")
    return jax.shard_map(body, mesh=mesh, in_specs=in_specs, out_specs=out_specs, check_vma=False)
```

```python
import jax
import jax.numpy as jnp
from jax import lax
from jax.sharding import PartitionSpec as P


HEAD_DIM = 128
BF = jnp.bfloat16
F32 = jnp.float32
WIDTH = 256
GROUP = 4


def rotate(values, positions):
    half_dim = values.shape[-1] // 2
    exponent = jnp.arange(half_dim, dtype=F32) * (2.0 / values.shape[-1])
    frequency = 500000.0 ** (-exponent)
    angles = positions.astype(F32)[:, None] * frequency[None, :]
    cosine = jnp.cos(angles)
    sine_part = jnp.sin(angles)
    first_half = values[..., :half_dim]
    second_half = values[..., half_dim:]
    return jnp.concatenate(
        [
            first_half * cosine - second_half * sine_part,
            second_half * cosine + first_half * sine_part,
        ],
        axis=-1,
    )


def flip_blocks(x, b):
    view = x.reshape(x.shape[0] // (2 * b), 2, b, *x.shape[1:])
    return view[:, ::-1].reshape(x.shape)


class Grid:
    def __init__(self):
        self.C = lax.axis_size("ctx")
        self.M = lax.axis_size("mp")
        self.c = lax.axis_index("ctx")
        self.m = lax.axis_index("mp")
        self.H = self.C // self.M
        self.far_bits = []
        bit = 2
        while bit < self.C:
            self.far_bits.append(bit)
            bit *= 2
        self.even = list(range(0, self.C, 2))
        self.order = self.even + [i + 1 for i in self.even]

    def bit(self, b):
        return (self.c // b) % 2

    def swap(self, x, b):
        return lax.ppermute(x, "ctx", [(i, i ^ b) for i in range(self.C)])

    def flat(self, pairs):
        return [(a * self.M + b, d * self.M + e) for (a, b), (d, e) in pairs]

    def rotate_mp(self, block_for):
        return [
            lax.ppermute(block_for(s), "mp", [(i, (i + s) % self.M) for i in range(self.M)])
            for s in range(1, self.M)
        ]

    def mp_sum(self, x):
        total = x
        for other in self.rotate_mp(lambda s: x):
            total = total + other
        return total

    def far_gather(self, x, bits):
        have = {0: x}
        for b in bits:
            keys = list(have)
            got = self.swap(jnp.stack([have[k] for k in keys]), b)
            for j, k in enumerate(keys):
                have[k ^ b] = got[j]
        return have

    def gather(self, parts):
        a = self.far_gather(parts[0], self.far_bits)
        b = self.far_gather(parts[1], self.far_bits[::-1])
        near = jnp.concatenate(
            [jnp.concatenate([a[i], b[i]], axis=1) for i in self.even], axis=0
        )
        return jnp.concatenate([near, self.swap(near, 1)], axis=0)

    def small_gather(self, x):
        near = self.far_gather(x, self.far_bits)
        near = jnp.stack([near[i] for i in self.even])
        other = self.swap(near, 1)
        return jnp.stack([near, other], axis=1).reshape(self.C, *x.shape)

    def xor_order(self, x, value):
        b = 1
        while b < self.C:
            x = jnp.where((value // b) % 2 == 1, flip_blocks(x, b), x)
            b *= 2
        return x

    def far_halve(self, blocks, bits):
        for b in bits:
            keep = [k for k in blocks if not k & b]
            got = self.swap(jnp.stack([blocks[k ^ b] for k in keep]).astype(BF), b)
            blocks = {k: blocks[k] + got[j].astype(F32) for j, k in enumerate(keep)}
        return blocks[0]

    def scatter_sum(self, near, far):
        half = near.shape[1] // 2
        n = near.shape[0] // len(self.even)
        near = near + self.swap(far.astype(BF), 1).astype(F32)
        parts = []
        for cols, bits in (
            (slice(0, half), self.far_bits[::-1]),
            (slice(half, None), self.far_bits),
        ):
            blocks = {i: near[j * n : (j + 1) * n, cols] for j, i in enumerate(self.even)}
            parts.append(self.far_halve(blocks, bits))
        return jnp.concatenate(parts, axis=1)

    def rows_to_slices(self, local_rows):
        n = local_rows.shape[0]
        f = local_rows.shape[1] // self.H
        payload = [
            lax.dynamic_slice(local_rows, (0, ((self.c % self.H) ^ i) * f), (n, f))
            for i in range(self.H)
        ]
        blocks = []
        for r in range(self.C):
            pairs = [
                ((a, b), (self.H * b + (a ^ r) % self.H, (a ^ r) // self.H))
                for a in range(self.C)
                for b in range(self.M)
            ]
            blocks.append(lax.ppermute(payload[r % self.H], ("ctx", "mp"), self.flat(pairs)))
        b = 1
        while b < self.H:
            swapped = self.bit(b) == 1
            blocks = [jnp.where(swapped, blocks[r ^ b], blocks[r]) for r in range(self.C)]
            b *= 2
        return blocks

    def slices_to_rows(self, partial):
        n = partial.shape[0] // self.C
        f = partial.shape[1]
        first = self.H * self.m
        full = jnp.zeros((self.C, n, f), BF)
        for r in range(self.C):
            got = lax.dynamic_slice(partial, (((self.c ^ r) ^ first) * n, 0), (n, f))
            if r:
                got = self.swap(got, r)
            full = lax.dynamic_update_slice(full, got[None], (self.c ^ r, 0, 0))

        def share(s):
            return lax.dynamic_slice(full, ((self.m + s) % self.M * self.H, 0, 0), (self.H, n, f))

        total = share(0).astype(F32)
        for got in self.rotate_mp(share):
            total = total + got.astype(F32)
        return [total[h] for h in range(self.H)]


def columns(weight, index):
    return lax.dynamic_slice(
        weight, (0, index * HEAD_DIM), (weight.shape[0], HEAD_DIM)
    )


def head_weights(grid, query_weight, key_weight, value_weight):
    group = grid.c // (grid.C // 2)
    odd = grid.bit(1) == 1
    mine = jnp.where(odd, value_weight, key_weight)
    other = jnp.where(odd, key_weight, value_weight)

    def side(near, kv):
        parts = []
        for g in range(2):
            parts += [columns(query_weight, grid.c ^ (i + near)) for i in grid.even[2 * g : 2 * g + 2]]
            parts.append(columns(kv, group ^ g))
        return jnp.concatenate(parts, axis=1)

    return side(1, other), side(0, mine)


def head_reduce(grid, send, keep, squares):
    d = HEAD_DIM
    other = grid.swap(send, 1)
    squares = squares + grid.swap(squares, 1)
    near = keep + other.astype(F32)
    half = near.shape[0] // 2
    group_bit = grid.C // 2
    side_bit = grid.far_bits[0]
    first, second = near[:half], near[half:]
    sq_a, sq_b = squares[:half], squares[half:]
    got_a = grid.swap(first[:, 3 * d :].astype(BF), group_bit).astype(F32)
    out = jnp.concatenate([second[:, d : 3 * d], second[:, 4 * d :]], axis=1).astype(BF)
    got_b = grid.swap(out, side_bit).astype(F32)
    sq_a = sq_a + grid.swap(sq_a, group_bit)
    sq_b = sq_b + grid.swap(sq_b, side_bit)
    a = first[:, : 3 * d] + got_a
    b0 = second[:, :d] + got_b[:, :d]
    bg0 = second[:, 2 * d : 3 * d] + got_b[:, d : 2 * d]
    b4 = second[:, 3 * d : 4 * d] + got_b[:, 2 * d : 3 * d]
    bg1 = second[:, 5 * d :] + got_b[:, 3 * d :]
    got_a = grid.swap(a[:, d:].astype(BF), side_bit).astype(F32)
    got_b = grid.swap(jnp.concatenate([b4, bg1], axis=1).astype(BF), group_bit).astype(F32)
    sq_a = sq_a + grid.swap(sq_a, side_bit)
    sq_b = sq_b + grid.swap(sq_b, group_bit)
    query = jnp.concatenate([a[:, :d] + got_a[:, :d], b0 + got_b[:, :d]], axis=0)
    own = jnp.concatenate([a[:, 2 * d :] + got_a[:, d:], bg0 + got_b[:, d:]], axis=0)
    return query, own, jnp.concatenate([sq_a, sq_b])


def feed_forward(grid, normed, gate_weight, up_weight, down_weight):
    C, M = grid.C, grid.M
    rows = normed.shape[0]
    hidden_cols = gate_weight.shape[1]
    width = WIDTH if hidden_cols % WIDTH == 0 else HEAD_DIM
    count = hidden_cols // width
    streams = 2
    place = jnp.where(grid.c % 2 == 1, grid.m, M - 1 - grid.m)

    def at(a, p):
        return (a, p if a % 2 == 1 else M - 1 - p)

    inward = grid.flat([(at(a, p), at(a, p + 1)) for a in range(C) for p in range(M - 1)])
    outward = grid.flat([(at(a, p + 1), at(a, p)) for a in range(C) for p in range(M - 1)])

    def choose(options):
        return lax.select_n(place, *options)

    partial = {}

    def part(k):
        if k not in partial:
            lo, hi = k * width, (k + 1) * width
            g = jnp.dot(normed, gate_weight[:, lo:hi], preferred_element_type=F32)
            u = jnp.dot(normed, up_weight[:, lo:hi], preferred_element_type=F32)
            partial[k] = jnp.concatenate([g.astype(BF), u.astype(BF)], axis=1)
        return partial[k]

    lists = [list(range(s, count, streams)) for s in range(streams)]
    got = [None] * streams
    passed = [None] * streams
    hist = [[] for _ in range(streams)]
    hids = [[] for _ in range(streams)]
    waiting = []
    total = None
    zero = jnp.zeros((rows, 2 * width), BF)
    tick = normed[:8, :128].astype(F32) * 0.0
    last = max(len(ks) for ks in lists) + 2 * (M - 1) - 1
    for t in range(last + 1):
        for s in range(streams):
            ks = lists[s]
            n = len(ks)
            came = got[s]
            if t < n + M - 2:
                options = [part(ks[t - p]) if 0 <= t - p < n else zero for p in range(M - 1)]
                own = choose(options + [zero])
                send = own if came is None else (own.astype(F32) + came.astype(F32)).astype(BF)
                got[s] = lax.ppermute(send, ("ctx", "mp"), inward)
            i = t - (M - 1)
            if 0 <= i < n + M - 2:
                if i < n:
                    full = came.astype(F32) + part(ks[i]).astype(F32)
                    g, u = full[:, :width], full[:, width:]
                    hids[s].append((jax.nn.silu(g) * u).astype(BF))
                fresh = hids[s][i] if i < n else jnp.zeros((rows, width), BF)
                send = fresh if passed[s] is None else jnp.where(place == M - 1, fresh, passed[s])
                passed[s] = lax.ppermute(send, ("ctx", "mp"), outward)
                hist[s].append(passed[s])
            j = i - (M - 2) - 1
            if 0 <= j < n:
                waiting.append(
                    (ks[j], choose([hist[s][j + M - 2 - p] for p in range(M - 1)] + [hids[s][j]]))
                )
            tick = tick * 0.5
            tick = lax.optimization_barrier(tick)
            final = t == last and s == streams - 1
            if len(waiting) >= GROUP or (final and waiting):
                waiting.sort(key=lambda kv: kv[0])
                k0, k1 = waiting[0][0], waiting[-1][0] + 1
                assert k1 - k0 == len(waiting)
                block = lax.optimization_barrier(jnp.concatenate([b for _, b in waiting], axis=1))
                waiting.clear()
                weight = down_weight[k0 * width : k1 * width]
                if final:
                    half = rows // 2
                    far = jnp.dot(block[half:], weight, preferred_element_type=F32)
                    near = jnp.dot(block[:half], weight, preferred_element_type=F32)
                    if total is not None:
                        far = far + total[half:]
                        near = near + total[:half]
                else:
                    piece = jnp.dot(block, weight, preferred_element_type=F32)
                    total = lax.optimization_barrier(piece if total is None else total + piece)
    return near, far, tick[0, 0]


def body(
    tokens,
    norm_gain,
    router_weight,
    query_weight,
    key_weight,
    value_weight,
    out_weight,
    mlp_gain,
    gate_weight,
    up_weight,
    down_weight,
    destination,
    kept_pos,
):
    grid = Grid()
    ctx_count, mp_count = grid.C, grid.M
    my_index = grid.c
    tok_dev = tokens.shape[0]
    kept_dev = kept_pos.shape[0]
    rows = kept_dev * ctx_count
    feature_cols = tokens.shape[1]
    feature_total = feature_cols * mp_count
    slice_cols = feature_total // ctx_count
    capacity = (3 * kept_dev // 2 + ctx_count - 1) // ctx_count
    slots_all = ctx_count * capacity
    head_dim = HEAD_DIM
    query_cols = query_weight.shape[1]
    key_cols = key_weight.shape[1]
    kv_local = key_cols // head_dim
    q_local = query_cols // head_dim
    group_size = q_local // kv_local
    peer_ids = jnp.arange(ctx_count, dtype=jnp.int32)
    is_kept = destination >= 0
    owner_ids = destination // kept_dev
    slot_ids = destination % kept_dev
    kept_order = slot_ids * ctx_count + owner_ids
    first_order = jnp.min(jnp.where(is_kept, kept_order, ctx_count * kept_dev))
    first_slots = (first_order - peer_ids + ctx_count - 1) // ctx_count
    owner_match = owner_ids[:, None] == peer_ids[None, :]
    send_index = (
        owner_ids * capacity
        + slot_ids
        - jnp.sum(jnp.where(owner_match, first_slots[None, :], 0), axis=1)
    )
    send_index = jnp.where(is_kept, send_index, slots_all)
    slot_ids_all = jnp.arange(slots_all, dtype=jnp.int32)
    takes = (slot_ids_all[:, None] == send_index[None, :]).astype(BF)
    outgoing = (
        jnp.dot(takes, tokens, preferred_element_type=F32)
        .astype(BF)
        .reshape(ctx_count, capacity, feature_cols)
    )
    incoming = lax.all_to_all(outgoing, "ctx", split_axis=0, concat_axis=0, tiled=True).reshape(
        slots_all, feature_cols
    )
    slot_range = jnp.arange(kept_dev, dtype=jnp.int32)
    source_ids = kept_pos // tok_dev
    source_match = source_ids[:, None] == peer_ids[None, :]
    first_from = jnp.min(jnp.where(source_match, slot_range[:, None], kept_dev), axis=0)
    recv_index = (
        source_ids * capacity
        + slot_range
        - jnp.sum(jnp.where(source_match, first_from[None, :], 0), axis=1)
    )
    local_rows = incoming[recv_index]
    fits = q_local == ctx_count and kv_local == 2 and len(grid.far_bits) == 2
    positions = grid.small_gather(kept_pos.astype(F32))
    local_rows, positions = lax.optimization_barrier((local_rows, positions))
    pos_all = grid.xor_order(positions, my_index ^ (grid.H * grid.m)).reshape(rows)
    blocks = grid.rows_to_slices(local_rows)
    raw_share = local_rows.astype(F32)
    my_router = lax.dynamic_slice(router_weight, (grid.m * feature_cols,), (feature_cols,))
    square_part = jnp.concatenate([jnp.sum(b.astype(F32) ** 2, axis=1) for b in blocks])
    my_gain = lax.dynamic_slice(norm_gain, (my_index * slice_cols,), (slice_cols,))
    my_gain = my_gain.astype(F32)[None, :]
    scaled = jnp.concatenate([(b.astype(F32) * my_gain).astype(BF) for b in blocks], axis=0)
    softmax_scale = head_dim ** (-0.5)
    if fits:
        send_weight, keep_weight = head_weights(grid, query_weight, key_weight, value_weight)
        out_rows = jnp.concatenate(
            [
                lax.dynamic_slice(
                    out_weight, ((my_index ^ i) * head_dim, 0), (head_dim, out_weight.shape[1])
                )
                for i in grid.order
            ],
            axis=0,
        )
        send = jnp.dot(scaled, send_weight, preferred_element_type=F32).astype(BF)
        keep = jnp.dot(scaled, keep_weight, preferred_element_type=F32)
        query, own, square_sum = head_reduce(grid, send, keep, square_part)
        inverse_all = lax.rsqrt(square_sum / feature_total + 1e-05)
        query = rotate(query * inverse_all[:, None], pos_all).astype(BF)
        own = own * inverse_all[:, None]
        even = grid.bit(1) == 0
        own = jnp.where(even, rotate(own, pos_all), own).astype(BF)
        other = grid.swap(own, 1)
        keys = jnp.where(even, own, other)
        values = jnp.where(even, other, own)
        allowed = pos_all[None, :] <= pos_all[:, None]
        scores = (
            lax.dot_general(query, keys, (((1,), (1,)), ((), ())), preferred_element_type=F32)
            * softmax_scale
        )
        scores = jnp.where(allowed, scores, -1e30)
        peak = jnp.max(scores, axis=-1, keepdims=True)
        weights = jnp.where(allowed, jnp.exp(scores - peak), 0.0)
        weighted = jnp.dot(weights, values.astype(F32))
        attended = (weighted / jnp.sum(weights, axis=-1, keepdims=True)).astype(BF)
        half = rows // 2
        first = grid.far_gather(attended[:half], grid.far_bits)
        second = grid.far_gather(attended[half:], grid.far_bits[::-1])
        near = jnp.concatenate(
            [jnp.concatenate([first[i], second[i]], axis=0) for i in grid.even], axis=1
        )
        span = len(grid.even) * head_dim
        partial_cols = jnp.dot(near, out_rows[:span], preferred_element_type=F32) + jnp.dot(
            grid.swap(near, 1), out_rows[span:], preferred_element_type=F32
        )
    else:
        stacked = jnp.concatenate([query_weight, key_weight, value_weight], axis=1)
        projected = jnp.dot(scaled, stacked, preferred_element_type=F32)
        mine = lax.psum_scatter(projected, "ctx", scatter_dimension=0, tiled=True)
        square_sum = lax.psum_scatter(square_part, "ctx", scatter_dimension=0, tiled=True)
        my_inverse = lax.rsqrt(square_sum / feature_total + 1e-05)
        my_pos = lax.dynamic_slice(pos_all, (my_index * kept_dev,), (kept_dev,))
        mine = mine * my_inverse[:, None]
        by_head = mine.reshape(kept_dev, q_local + 2 * kv_local, head_dim).transpose(1, 0, 2)
        queries = rotate(by_head[:q_local], my_pos).astype(BF)
        queries = queries.reshape(kv_local, group_size, kept_dev, head_dim)
        keys = rotate(by_head[q_local : q_local + kv_local], my_pos).astype(BF)
        values = by_head[q_local + kv_local :].astype(BF)
        keys = lax.all_gather(keys, "ctx", axis=1, tiled=True)
        values = lax.all_gather(values, "ctx", axis=1, tiled=True)
        allowed = pos_all[None, :] <= my_pos[:, None]
        scores = (
            jnp.einsum("hgqd,hkd->hgqk", queries, keys, preferred_element_type=F32) * softmax_scale
        )
        scores = jnp.where(allowed, scores, -1e30)
        peak = jnp.max(scores, axis=-1, keepdims=True)
        weights = jnp.where(allowed, jnp.exp(scores - peak), 0.0)
        weighted = jnp.einsum("hgqk,hkd->hgqd", weights, values.astype(F32))
        attended = weighted / jnp.sum(weights, axis=-1, keepdims=True)
        attended = attended.transpose(2, 0, 1, 3).reshape(kept_dev, query_cols).astype(BF)
        every_head = lax.all_gather(attended, "ctx", axis=0, tiled=True)
        partial_cols = jnp.dot(every_head, out_weight, preferred_element_type=F32)
    head_share = jnp.concatenate(grid.slices_to_rows(partial_cols.astype(BF)), axis=1)
    mixed_share = raw_share + head_share
    sums = grid.mp_sum(
        jnp.stack(
            [
                jnp.sum(mixed_share * mixed_share, axis=1),
                jnp.sum(raw_share * my_router.astype(F32)[None, :], axis=1),
            ]
        )
    )
    router_score = jax.nn.sigmoid(sums[1])
    second_inverse = lax.rsqrt(sums[0] / feature_total + 1e-05)[:, None]
    second_scaled = (mixed_share * second_inverse * mlp_gain.astype(F32)).astype(BF)
    mid = feature_cols // 2
    every_scaled = grid.gather((second_scaled[:, :mid], second_scaled[:, mid:]))
    near, far, tick = feed_forward(
        grid, every_scaled, gate_weight, up_weight, down_weight
    )
    mlp_share = grid.scatter_sum(near, far)
    update = (router_score[:, None] * (head_share + mlp_share) + tick).astype(BF)
    places = (slot_ids_all[:, None] == recv_index[None, :]).astype(BF)
    returning = (
        jnp.dot(places, update, preferred_element_type=F32)
        .astype(BF)
        .reshape(ctx_count, capacity, feature_cols)
    )
    returned = lax.all_to_all(returning, "ctx", split_axis=0, concat_axis=0, tiled=True).reshape(
        slots_all, feature_cols
    )
    lands = (send_index[:, None] == slot_ids_all[None, :]).astype(BF)
    arriving = jnp.dot(lands, returned, preferred_element_type=F32)
    return (tokens.astype(F32) + arriving).astype(BF)


def solution(mesh):
    in_specs = (
        P("ctx", "mp"),
        P(),
        P(),
        P("ctx", "mp"),
        P("ctx", "mp"),
        P("ctx", "mp"),
        P("mp", "ctx"),
        P("mp"),
        P("mp", "ctx"),
        P("mp", "ctx"),
        P("ctx", "mp"),
        P("ctx"),
        P("ctx"),
    )
    out_specs = P("ctx", "mp")
    return jax.shard_map(body, mesh=mesh, in_specs=in_specs, out_specs=out_specs, check_vma=False)
```

```python
import jax
import jax.numpy as jnp
from jax import lax
from jax.sharding import PartitionSpec as P


HEAD_DIM = 128
BF = jnp.bfloat16
F32 = jnp.float32
WIDTH = 256
GROUP = 4


def rotate(values, positions):
    half_dim = values.shape[-1] // 2
    exponent = jnp.arange(half_dim, dtype=F32) * (2.0 / values.shape[-1])
    frequency = 500000.0 ** (-exponent)
    angles = positions.astype(F32)[:, None] * frequency[None, :]
    cosine = jnp.cos(angles)
    sine_part = jnp.sin(angles)
    first_half = values[..., :half_dim]
    second_half = values[..., half_dim:]
    return jnp.concatenate(
        [
            first_half * cosine - second_half * sine_part,
            second_half * cosine + first_half * sine_part,
        ],
        axis=-1,
    )


def flip_blocks(x, b):
    view = x.reshape(x.shape[0] // (2 * b), 2, b, *x.shape[1:])
    return view[:, ::-1].reshape(x.shape)


class Grid:
    def __init__(self):
        self.C = lax.axis_size("ctx")
        self.M = lax.axis_size("mp")
        self.c = lax.axis_index("ctx")
        self.m = lax.axis_index("mp")
        self.H = self.C // self.M
        self.far_bits = []
        bit = 2
        while bit < self.C:
            self.far_bits.append(bit)
            bit *= 2
        self.even = list(range(0, self.C, 2))
        self.order = self.even + [i + 1 for i in self.even]

    def bit(self, b):
        return (self.c // b) % 2

    def swap(self, x, b):
        return lax.ppermute(x, "ctx", [(i, i ^ b) for i in range(self.C)])

    def flat(self, pairs):
        return [(a * self.M + b, d * self.M + e) for (a, b), (d, e) in pairs]

    def rotate_mp(self, block_for):
        return [
            lax.ppermute(block_for(s), "mp", [(i, (i + s) % self.M) for i in range(self.M)])
            for s in range(1, self.M)
        ]

    def mp_sum(self, x):
        total = x
        for other in self.rotate_mp(lambda s: x):
            total = total + other
        return total

    def far_gather(self, x, bits):
        have = {0: x}
        for b in bits:
            keys = list(have)
            got = self.swap(jnp.stack([have[k] for k in keys]), b)
            for j, k in enumerate(keys):
                have[k ^ b] = got[j]
        return have

    def gather(self, parts):
        a = self.far_gather(parts[0], self.far_bits)
        b = self.far_gather(parts[1], self.far_bits[::-1])
        near = jnp.concatenate(
            [jnp.concatenate([a[i], b[i]], axis=1) for i in self.even], axis=0
        )
        return jnp.concatenate([near, self.swap(near, 1)], axis=0)

    def small_gather(self, x):
        near = self.far_gather(x, self.far_bits)
        near = jnp.stack([near[i] for i in self.even])
        other = self.swap(near, 1)
        return jnp.stack([near, other], axis=1).reshape(self.C, *x.shape)

    def xor_order(self, x, value):
        b = 1
        while b < self.C:
            x = jnp.where((value // b) % 2 == 1, flip_blocks(x, b), x)
            b *= 2
        return x

    def far_halve(self, blocks, bits):
        for b in bits:
            keep = [k for k in blocks if not k & b]
            got = self.swap(jnp.stack([blocks[k ^ b] for k in keep]).astype(BF), b)
            blocks = {k: blocks[k] + got[j].astype(F32) for j, k in enumerate(keep)}
        return blocks[0]

    def scatter_sum(self, near, far):
        half = near.shape[1] // 2
        n = near.shape[0] // len(self.even)
        near = near + self.swap(far.astype(BF), 1).astype(F32)
        parts = []
        for cols, bits in (
            (slice(0, half), self.far_bits[::-1]),
            (slice(half, None), self.far_bits),
        ):
            blocks = {i: near[j * n : (j + 1) * n, cols] for j, i in enumerate(self.even)}
            parts.append(self.far_halve(blocks, bits))
        return jnp.concatenate(parts, axis=1)

    def rows_to_slices(self, local_rows):
        n = local_rows.shape[0]
        f = local_rows.shape[1] // self.H
        payload = [
            lax.dynamic_slice(local_rows, (0, ((self.c % self.H) ^ i) * f), (n, f))
            for i in range(self.H)
        ]
        blocks = []
        for r in range(self.C):
            pairs = [
                ((a, b), (self.H * b + (a ^ r) % self.H, (a ^ r) // self.H))
                for a in range(self.C)
                for b in range(self.M)
            ]
            blocks.append(lax.ppermute(payload[r % self.H], ("ctx", "mp"), self.flat(pairs)))
        b = 1
        while b < self.H:
            swapped = self.bit(b) == 1
            blocks = [jnp.where(swapped, blocks[r ^ b], blocks[r]) for r in range(self.C)]
            b *= 2
        return blocks

    def slices_to_rows(self, partial):
        n = partial.shape[0] // self.C
        f = partial.shape[1]
        first = self.H * self.m
        full = jnp.zeros((self.C, n, f), BF)
        for r in range(self.C):
            got = lax.dynamic_slice(partial, (((self.c ^ r) ^ first) * n, 0), (n, f))
            if r:
                got = self.swap(got, r)
            full = lax.dynamic_update_slice(full, got[None], (self.c ^ r, 0, 0))

        def share(s):
            return lax.dynamic_slice(full, ((self.m + s) % self.M * self.H, 0, 0), (self.H, n, f))

        total = share(0).astype(F32)
        for got in self.rotate_mp(share):
            total = total + got.astype(F32)
        return [total[h] for h in range(self.H)]


def columns(weight, index):
    return lax.dynamic_slice(
        weight, (0, index * HEAD_DIM), (weight.shape[0], HEAD_DIM)
    )


def head_weights(grid, query_weight, key_weight, value_weight):
    group = grid.c // (grid.C // 2)
    odd = grid.bit(1) == 1
    mine = jnp.where(odd, value_weight, key_weight)
    other = jnp.where(odd, key_weight, value_weight)

    def side(near, kv):
        parts = []
        for g in range(2):
            parts += [columns(query_weight, grid.c ^ (i + near)) for i in grid.even[2 * g : 2 * g + 2]]
            parts.append(columns(kv, group ^ g))
        return jnp.concatenate(parts, axis=1)

    return side(1, other), side(0, mine)


def head_reduce(grid, send, keep, squares):
    d = HEAD_DIM
    other = grid.swap(send, 1)
    squares = squares + grid.swap(squares, 1)
    near = keep + other.astype(F32)
    half = near.shape[0] // 2
    group_bit = grid.C // 2
    side_bit = grid.far_bits[0]
    first, second = near[:half], near[half:]
    sq_a, sq_b = squares[:half], squares[half:]
    got_a = grid.swap(first[:, 3 * d :].astype(BF), group_bit).astype(F32)
    out = jnp.concatenate([second[:, d : 3 * d], second[:, 4 * d :]], axis=1).astype(BF)
    got_b = grid.swap(out, side_bit).astype(F32)
    sq_a = sq_a + grid.swap(sq_a, group_bit)
    sq_b = sq_b + grid.swap(sq_b, side_bit)
    a = first[:, : 3 * d] + got_a
    b0 = second[:, :d] + got_b[:, :d]
    bg0 = second[:, 2 * d : 3 * d] + got_b[:, d : 2 * d]
    b4 = second[:, 3 * d : 4 * d] + got_b[:, 2 * d : 3 * d]
    bg1 = second[:, 5 * d :] + got_b[:, 3 * d :]
    got_a = grid.swap(a[:, d:].astype(BF), side_bit).astype(F32)
    got_b = grid.swap(jnp.concatenate([b4, bg1], axis=1).astype(BF), group_bit).astype(F32)
    sq_a = sq_a + grid.swap(sq_a, side_bit)
    sq_b = sq_b + grid.swap(sq_b, group_bit)
    query = jnp.concatenate([a[:, :d] + got_a[:, :d], b0 + got_b[:, :d]], axis=0)
    own = jnp.concatenate([a[:, 2 * d :] + got_a[:, d:], bg0 + got_b[:, d:]], axis=0)
    return query, own, jnp.concatenate([sq_a, sq_b])


def feed_forward(grid, normed, gate_weight, up_weight, down_weight):
    C, M = grid.C, grid.M
    rows = normed.shape[0]
    hidden_cols = gate_weight.shape[1]
    width = WIDTH if hidden_cols % WIDTH == 0 else HEAD_DIM
    count = hidden_cols // width
    streams = 2
    place = jnp.where(grid.c % 2 == 1, grid.m, M - 1 - grid.m)

    def at(a, p):
        return (a, p if a % 2 == 1 else M - 1 - p)

    inward = grid.flat([(at(a, p), at(a, p + 1)) for a in range(C) for p in range(M - 1)])
    outward = grid.flat([(at(a, p + 1), at(a, p)) for a in range(C) for p in range(M - 1)])

    def choose(options):
        return lax.select_n(place, *options)

    partial = {}

    def part(k):
        if k not in partial:
            lo, hi = k * width, (k + 1) * width
            g = jnp.dot(normed, gate_weight[:, lo:hi], preferred_element_type=F32)
            u = jnp.dot(normed, up_weight[:, lo:hi], preferred_element_type=F32)
            partial[k] = jnp.concatenate([g.astype(BF), u.astype(BF)], axis=1)
        return partial[k]

    lists = [list(range(s, count, streams)) for s in range(streams)]
    got = [None] * streams
    passed = [None] * streams
    hist = [[] for _ in range(streams)]
    hids = [[] for _ in range(streams)]
    waiting = []
    taken = 0
    total = None
    zero = jnp.zeros((rows, 2 * width), BF)
    tick = normed[:8, :128].astype(F32) * 0.0
    last = max(len(ks) for ks in lists) + 2 * (M - 1) - 2
    straight = [[] for _ in range(streams)]
    for t in range(last + 1):
        for s in range(streams):
            ks = lists[s]
            n = len(ks)
            came = got[s]
            if t < n + M - 2:
                options = [part(ks[t - p]) if 0 <= t - p < n else zero for p in range(M - 1)]
                own = choose(options + [zero])
                send = own if came is None else (own.astype(F32) + came.astype(F32)).astype(BF)
                got[s] = lax.ppermute(send, ("ctx", "mp"), inward)
            i = t - (M - 1)
            if 0 <= i < n:
                full = came.astype(F32) + part(ks[i]).astype(F32)
                g, u = full[:, :width], full[:, width:]
                hids[s].append((jax.nn.silu(g) * u).astype(BF))
            if 0 <= i < n - 1 + M - 2:
                fresh = hids[s][i] if i < n - 1 else jnp.zeros((rows, width), BF)
                send = fresh if passed[s] is None else jnp.where(place == M - 1, fresh, passed[s])
                passed[s] = lax.ppermute(send, ("ctx", "mp"), outward)
                hist[s].append(passed[s])
            if i == n - 1:
                for d in reversed(range(1, M)):
                    pairs = grid.flat([(at(a, M - 1), at(a, M - 1 - d)) for a in range(C)])
                    straight[s].append(lax.ppermute(hids[s][i], ("ctx", "mp"), pairs))
            j = i - (M - 2) - 1
            if 0 <= j < n - 1:
                waiting.append(
                    (ks[j], choose([hist[s][j + M - 2 - p] for p in range(M - 1)] + [hids[s][j]]))
                )
            if i == n + M - 3:
                waiting.append((ks[n - 1], choose(straight[s] + [hids[s][n - 1]])))
            tick = tick * 0.5
            tick = lax.optimization_barrier(tick)
            final = taken + len(waiting) == count
            waiting.sort(key=lambda kv: kv[0])
            run = bool(waiting) and waiting[-1][0] - waiting[0][0] == len(waiting) - 1
            if waiting and ((len(waiting) >= GROUP and run) or final):
                taken += len(waiting)
                k0, k1 = waiting[0][0], waiting[-1][0] + 1
                block = lax.optimization_barrier(jnp.concatenate([b for _, b in waiting], axis=1))
                waiting.clear()
                weight = down_weight[k0 * width : k1 * width]
                if final:
                    half = rows // 2
                    far = jnp.dot(block[half:], weight, preferred_element_type=F32)
                    near = jnp.dot(block[:half], weight, preferred_element_type=F32)
                    if total is not None:
                        far = far + total[half:]
                        near = near + total[:half]
                else:
                    piece = jnp.dot(block, weight, preferred_element_type=F32)
                    total = lax.optimization_barrier(piece if total is None else total + piece)
    return near, far, tick[0, 0]


def body(
    tokens,
    norm_gain,
    router_weight,
    query_weight,
    key_weight,
    value_weight,
    out_weight,
    mlp_gain,
    gate_weight,
    up_weight,
    down_weight,
    destination,
    kept_pos,
):
    grid = Grid()
    ctx_count, mp_count = grid.C, grid.M
    my_index = grid.c
    tok_dev = tokens.shape[0]
    kept_dev = kept_pos.shape[0]
    rows = kept_dev * ctx_count
    feature_cols = tokens.shape[1]
    feature_total = feature_cols * mp_count
    slice_cols = feature_total // ctx_count
    capacity = (3 * kept_dev // 2 + ctx_count - 1) // ctx_count
    slots_all = ctx_count * capacity
    head_dim = HEAD_DIM
    query_cols = query_weight.shape[1]
    key_cols = key_weight.shape[1]
    kv_local = key_cols // head_dim
    q_local = query_cols // head_dim
    group_size = q_local // kv_local
    peer_ids = jnp.arange(ctx_count, dtype=jnp.int32)
    is_kept = destination >= 0
    owner_ids = destination // kept_dev
    slot_ids = destination % kept_dev
    kept_order = slot_ids * ctx_count + owner_ids
    first_order = jnp.min(jnp.where(is_kept, kept_order, ctx_count * kept_dev))
    first_slots = (first_order - peer_ids + ctx_count - 1) // ctx_count
    owner_match = owner_ids[:, None] == peer_ids[None, :]
    send_index = (
        owner_ids * capacity
        + slot_ids
        - jnp.sum(jnp.where(owner_match, first_slots[None, :], 0), axis=1)
    )
    send_index = jnp.where(is_kept, send_index, slots_all)
    slot_ids_all = jnp.arange(slots_all, dtype=jnp.int32)
    takes = (slot_ids_all[:, None] == send_index[None, :]).astype(BF)
    outgoing = (
        jnp.dot(takes, tokens, preferred_element_type=F32)
        .astype(BF)
        .reshape(ctx_count, capacity, feature_cols)
    )
    incoming = lax.all_to_all(outgoing, "ctx", split_axis=0, concat_axis=0, tiled=True).reshape(
        slots_all, feature_cols
    )
    slot_range = jnp.arange(kept_dev, dtype=jnp.int32)
    source_ids = kept_pos // tok_dev
    source_match = source_ids[:, None] == peer_ids[None, :]
    first_from = jnp.min(jnp.where(source_match, slot_range[:, None], kept_dev), axis=0)
    recv_index = (
        source_ids * capacity
        + slot_range
        - jnp.sum(jnp.where(source_match, first_from[None, :], 0), axis=1)
    )
    local_rows = incoming[recv_index]
    fits = q_local == ctx_count and kv_local == 2 and len(grid.far_bits) == 2
    positions = grid.small_gather(kept_pos.astype(F32))
    local_rows, positions = lax.optimization_barrier((local_rows, positions))
    pos_all = grid.xor_order(positions, my_index ^ (grid.H * grid.m)).reshape(rows)
    blocks = grid.rows_to_slices(local_rows)
    raw_share = local_rows.astype(F32)
    my_router = lax.dynamic_slice(router_weight, (grid.m * feature_cols,), (feature_cols,))
    square_part = jnp.concatenate([jnp.sum(b.astype(F32) ** 2, axis=1) for b in blocks])
    my_gain = lax.dynamic_slice(norm_gain, (my_index * slice_cols,), (slice_cols,))
    my_gain = my_gain.astype(F32)[None, :]
    scaled = jnp.concatenate([(b.astype(F32) * my_gain).astype(BF) for b in blocks], axis=0)
    softmax_scale = head_dim ** (-0.5)
    if fits:
        send_weight, keep_weight = head_weights(grid, query_weight, key_weight, value_weight)
        out_rows = jnp.concatenate(
            [
                lax.dynamic_slice(
                    out_weight, ((my_index ^ i) * head_dim, 0), (head_dim, out_weight.shape[1])
                )
                for i in grid.order
            ],
            axis=0,
        )
        send = jnp.dot(scaled, send_weight, preferred_element_type=F32).astype(BF)
        keep = jnp.dot(scaled, keep_weight, preferred_element_type=F32)
        keep = lax.optimization_barrier(keep)
        query, own, square_sum = head_reduce(grid, send, keep, square_part)
        inverse_all = lax.rsqrt(square_sum / feature_total + 1e-05)
        query = rotate(query * inverse_all[:, None], pos_all).astype(BF)
        own = own * inverse_all[:, None]
        even = grid.bit(1) == 0
        own = jnp.where(even, rotate(own, pos_all), own).astype(BF)
        other = grid.swap(own, 1)
        keys = jnp.where(even, own, other)
        values = jnp.where(even, other, own)
        allowed = pos_all[None, :] <= pos_all[:, None]
        scores = (
            lax.dot_general(query, keys, (((1,), (1,)), ((), ())), preferred_element_type=F32)
            * softmax_scale
        )
        scores = jnp.where(allowed, scores, -1e30)
        peak = jnp.max(scores, axis=-1, keepdims=True)
        weights = jnp.where(allowed, jnp.exp(scores - peak), 0.0)
        weighted = jnp.dot(weights, values.astype(F32))
        attended = (weighted / jnp.sum(weights, axis=-1, keepdims=True)).astype(BF)
        half = rows // 2
        first = grid.far_gather(attended[:half], grid.far_bits)
        second = grid.far_gather(attended[half:], grid.far_bits[::-1])
        near = jnp.concatenate(
            [jnp.concatenate([first[i], second[i]], axis=0) for i in grid.even], axis=1
        )
        span = len(grid.even) * head_dim
        partial_cols = jnp.dot(near, out_rows[:span], preferred_element_type=F32) + jnp.dot(
            grid.swap(near, 1), out_rows[span:], preferred_element_type=F32
        )
    else:
        stacked = jnp.concatenate([query_weight, key_weight, value_weight], axis=1)
        projected = jnp.dot(scaled, stacked, preferred_element_type=F32)
        mine = lax.psum_scatter(projected, "ctx", scatter_dimension=0, tiled=True)
        square_sum = lax.psum_scatter(square_part, "ctx", scatter_dimension=0, tiled=True)
        my_inverse = lax.rsqrt(square_sum / feature_total + 1e-05)
        my_pos = lax.dynamic_slice(pos_all, (my_index * kept_dev,), (kept_dev,))
        mine = mine * my_inverse[:, None]
        by_head = mine.reshape(kept_dev, q_local + 2 * kv_local, head_dim).transpose(1, 0, 2)
        queries = rotate(by_head[:q_local], my_pos).astype(BF)
        queries = queries.reshape(kv_local, group_size, kept_dev, head_dim)
        keys = rotate(by_head[q_local : q_local + kv_local], my_pos).astype(BF)
        values = by_head[q_local + kv_local :].astype(BF)
        keys = lax.all_gather(keys, "ctx", axis=1, tiled=True)
        values = lax.all_gather(values, "ctx", axis=1, tiled=True)
        allowed = pos_all[None, :] <= my_pos[:, None]
        scores = (
            jnp.einsum("hgqd,hkd->hgqk", queries, keys, preferred_element_type=F32) * softmax_scale
        )
        scores = jnp.where(allowed, scores, -1e30)
        peak = jnp.max(scores, axis=-1, keepdims=True)
        weights = jnp.where(allowed, jnp.exp(scores - peak), 0.0)
        weighted = jnp.einsum("hgqk,hkd->hgqd", weights, values.astype(F32))
        attended = weighted / jnp.sum(weights, axis=-1, keepdims=True)
        attended = attended.transpose(2, 0, 1, 3).reshape(kept_dev, query_cols).astype(BF)
        every_head = lax.all_gather(attended, "ctx", axis=0, tiled=True)
        partial_cols = jnp.dot(every_head, out_weight, preferred_element_type=F32)
    head_share = jnp.concatenate(grid.slices_to_rows(partial_cols.astype(BF)), axis=1)
    mixed_share = raw_share + head_share
    sums = grid.mp_sum(
        jnp.stack(
            [
                jnp.sum(mixed_share * mixed_share, axis=1),
                jnp.sum(raw_share * my_router.astype(F32)[None, :], axis=1),
            ]
        )
    )
    router_score = jax.nn.sigmoid(sums[1])
    second_inverse = lax.rsqrt(sums[0] / feature_total + 1e-05)[:, None]
    second_scaled = (mixed_share * second_inverse * mlp_gain.astype(F32)).astype(BF)
    mid = feature_cols // 2
    every_scaled = grid.gather((second_scaled[:, :mid], second_scaled[:, mid:]))
    near, far, tick = feed_forward(grid, every_scaled, gate_weight, up_weight, down_weight)
    mlp_share = grid.scatter_sum(near, far)
    update = (router_score[:, None] * (head_share + mlp_share) + tick).astype(BF)
    places = (slot_ids_all[:, None] == recv_index[None, :]).astype(BF)
    returning = (
        jnp.dot(places, update, preferred_element_type=F32)
        .astype(BF)
        .reshape(ctx_count, capacity, feature_cols)
    )
    returned = lax.all_to_all(returning, "ctx", split_axis=0, concat_axis=0, tiled=True).reshape(
        slots_all, feature_cols
    )
    lands = (send_index[:, None] == slot_ids_all[None, :]).astype(BF)
    arriving = jnp.dot(lands, returned, preferred_element_type=F32)
    return (tokens.astype(F32) + arriving).astype(BF)


def solution(mesh):
    in_specs = (
        P("ctx", "mp"),
        P(),
        P(),
        P("ctx", "mp"),
        P("ctx", "mp"),
        P("ctx", "mp"),
        P("mp", "ctx"),
        P("mp"),
        P("mp", "ctx"),
        P("mp", "ctx"),
        P("ctx", "mp"),
        P("ctx"),
        P("ctx"),
    )
    out_specs = P("ctx", "mp")

    return jax.shard_map(body, mesh=mesh, in_specs=in_specs, out_specs=out_specs, check_vma=False)
```

```python
import jax
import jax.numpy as jnp
from jax import lax
from jax.sharding import PartitionSpec as P


HEAD_DIM = 128
BF = jnp.bfloat16
F32 = jnp.float32
WIDTH = 256
GROUP = 4


def rotate(values, positions):
    half_dim = values.shape[-1] // 2
    exponent = jnp.arange(half_dim, dtype=F32) * (2.0 / values.shape[-1])
    frequency = 500000.0 ** (-exponent)
    angles = positions.astype(F32)[:, None] * frequency[None, :]
    cosine = jnp.cos(angles)
    sine_part = jnp.sin(angles)
    first_half = values[..., :half_dim]
    second_half = values[..., half_dim:]
    return jnp.concatenate(
        [
            first_half * cosine - second_half * sine_part,
            second_half * cosine + first_half * sine_part,
        ],
        axis=-1,
    )


def flip_blocks(x, b):
    view = x.reshape(x.shape[0] // (2 * b), 2, b, *x.shape[1:])
    return view[:, ::-1].reshape(x.shape)


class Grid:
    def __init__(self):
        self.C = lax.axis_size("ctx")
        self.M = lax.axis_size("mp")
        self.c = lax.axis_index("ctx")
        self.m = lax.axis_index("mp")
        self.H = self.C // self.M
        self.far_bits = []
        bit = 2
        while bit < self.C:
            self.far_bits.append(bit)
            bit *= 2
        self.even = list(range(0, self.C, 2))
        self.order = self.even + [i + 1 for i in self.even]

    def bit(self, b):
        return (self.c // b) % 2

    def swap(self, x, b):
        return lax.ppermute(x, "ctx", [(i, i ^ b) for i in range(self.C)])

    def flat(self, pairs):
        return [(a * self.M + b, d * self.M + e) for (a, b), (d, e) in pairs]

    def rotate_mp(self, block_for):
        return [
            lax.ppermute(block_for(s), "mp", [(i, (i + s) % self.M) for i in range(self.M)])
            for s in range(1, self.M)
        ]

    def mp_sum(self, x):
        total = x
        for other in self.rotate_mp(lambda s: x):
            total = total + other
        return total

    def far_gather(self, x, bits):
        have = {0: x}
        for b in bits:
            keys = list(have)
            got = self.swap(jnp.stack([have[k] for k in keys]), b)
            for j, k in enumerate(keys):
                have[k ^ b] = got[j]
        return have

    def gather(self, parts):
        a = self.far_gather(parts[0], self.far_bits)
        b = self.far_gather(parts[1], self.far_bits[::-1])
        near = jnp.concatenate(
            [jnp.concatenate([a[i], b[i]], axis=1) for i in self.even], axis=0
        )
        return jnp.concatenate([near, self.swap(near, 1)], axis=0)

    def small_gather(self, x):
        out = x[None]
        b = 1
        while b < self.C:
            out = jnp.concatenate([out, self.swap(out, b)])
            b *= 2
        return out

    def xor_order(self, x, value):
        b = 1
        while b < self.C:
            x = jnp.where((value // b) % 2 == 1, flip_blocks(x, b), x)
            b *= 2
        return x

    def far_halve(self, blocks, bits):
        for b in bits:
            keep = [k for k in blocks if not k & b]
            got = self.swap(jnp.stack([blocks[k ^ b] for k in keep]).astype(BF), b)
            blocks = {k: blocks[k] + got[j].astype(F32) for j, k in enumerate(keep)}
        return blocks[0]

    def scatter_sum(self, near, far):
        half = near.shape[1] // 2
        n = near.shape[0] // len(self.even)
        near = near + self.swap(far.astype(BF), 1).astype(F32)
        parts = []
        for cols, bits in (
            (slice(0, half), self.far_bits[::-1]),
            (slice(half, None), self.far_bits),
        ):
            blocks = {i: near[j * n : (j + 1) * n, cols] for j, i in enumerate(self.even)}
            parts.append(self.far_halve(blocks, bits))
        return jnp.concatenate(parts, axis=1)

    def rows_to_slices(self, local_rows):
        n = local_rows.shape[0]
        f = local_rows.shape[1] // self.H
        payload = [
            lax.dynamic_slice(local_rows, (0, ((self.c % self.H) ^ i) * f), (n, f))
            for i in range(self.H)
        ]
        blocks = []
        for r in range(self.C):
            pairs = [
                ((a, b), (self.H * b + (a ^ r) % self.H, (a ^ r) // self.H))
                for a in range(self.C)
                for b in range(self.M)
            ]
            blocks.append(lax.ppermute(payload[r % self.H], ("ctx", "mp"), self.flat(pairs)))
        b = 1
        while b < self.H:
            swapped = self.bit(b) == 1
            blocks = [jnp.where(swapped, blocks[r ^ b], blocks[r]) for r in range(self.C)]
            b *= 2
        return blocks

    def slices_to_rows(self, partial):
        n = partial.shape[0] // self.C
        f = partial.shape[1]
        first = self.H * self.m
        full = jnp.zeros((self.C, n, f), BF)
        for r in range(self.C):
            got = lax.dynamic_slice(partial, (((self.c ^ r) ^ first) * n, 0), (n, f))
            if r:
                got = self.swap(got, r)
            full = lax.dynamic_update_slice(full, got[None], (self.c ^ r, 0, 0))

        def share(s):
            return lax.dynamic_slice(full, ((self.m + s) % self.M * self.H, 0, 0), (self.H, n, f))

        total = share(0).astype(F32)
        for got in self.rotate_mp(share):
            total = total + got.astype(F32)
        return [total[h] for h in range(self.H)]


def columns(weight, index):
    return lax.dynamic_slice(
        weight, (0, index * HEAD_DIM), (weight.shape[0], HEAD_DIM)
    )


def head_weights(grid, query_weight, key_weight, value_weight):
    group = grid.c // (grid.C // 2)
    odd = grid.bit(1) == 1
    mine = jnp.where(odd, value_weight, key_weight)
    other = jnp.where(odd, key_weight, value_weight)

    def side(near, kv):
        parts = []
        for g in range(2):
            parts += [columns(query_weight, grid.c ^ (i + near)) for i in grid.even[2 * g : 2 * g + 2]]
            parts.append(columns(kv, group ^ g))
        return jnp.concatenate(parts, axis=1)

    return side(1, other), side(0, mine)


def head_reduce(grid, send, keep, squares):
    d = HEAD_DIM
    other = grid.swap(send, 1)
    squares = squares + grid.swap(squares, 1)
    near = keep + other.astype(F32)
    half = near.shape[0] // 2
    group_bit = grid.C // 2
    side_bit = grid.far_bits[0]
    first, second = near[:half], near[half:]
    sq_a, sq_b = squares[:half], squares[half:]
    out = jnp.concatenate([second[:, d : 3 * d], second[:, 4 * d :]], axis=1).astype(BF)
    got_a = grid.swap(first[:, 3 * d :].astype(BF), group_bit).astype(F32)
    got_b = grid.swap(out, side_bit).astype(F32)
    sq_a = sq_a + grid.swap(sq_a, group_bit)
    sq_b = sq_b + grid.swap(sq_b, side_bit)
    a = first[:, : 3 * d] + got_a
    b0 = second[:, :d] + got_b[:, :d]
    bg0 = second[:, 2 * d : 3 * d] + got_b[:, d : 2 * d]
    b4 = second[:, 3 * d : 4 * d] + got_b[:, 2 * d : 3 * d]
    bg1 = second[:, 5 * d :] + got_b[:, 3 * d :]
    got_a = grid.swap(a[:, d:].astype(BF), side_bit).astype(F32)
    got_b = grid.swap(jnp.concatenate([b4, bg1], axis=1).astype(BF), group_bit).astype(F32)
    sq_a = sq_a + grid.swap(sq_a, side_bit)
    sq_b = sq_b + grid.swap(sq_b, group_bit)
    query = jnp.concatenate([a[:, :d] + got_a[:, :d], b0 + got_b[:, :d]], axis=0)
    own = jnp.concatenate([a[:, 2 * d :] + got_a[:, d:], bg0 + got_b[:, d:]], axis=0)
    return query, own, jnp.concatenate([sq_a, sq_b])


def feed_forward(grid, normed, gate_weight, up_weight, down_weight):
    C, M = grid.C, grid.M
    rows = normed.shape[0]
    hidden_cols = gate_weight.shape[1]
    width = WIDTH if hidden_cols % WIDTH == 0 else HEAD_DIM
    count = hidden_cols // width
    streams = 2
    place = jnp.where(grid.c % 2 == 1, grid.m, M - 1 - grid.m)

    def at(a, p):
        return (a, p if a % 2 == 1 else M - 1 - p)

    inward = grid.flat([(at(a, p), at(a, p + 1)) for a in range(C) for p in range(M - 1)])
    outward = grid.flat([(at(a, p + 1), at(a, p)) for a in range(C) for p in range(M - 1)])

    def choose(options):
        return lax.select_n(place, *options)

    partial = {}

    def part(k):
        if k not in partial:
            lo, hi = k * width, (k + 1) * width
            g = jnp.dot(normed, gate_weight[:, lo:hi], preferred_element_type=F32)
            u = jnp.dot(normed, up_weight[:, lo:hi], preferred_element_type=F32)
            partial[k] = jnp.concatenate([g.astype(BF), u.astype(BF)], axis=1)
        return partial[k]

    lists = [list(range(s, count, streams)) for s in range(streams)]
    got = [None] * streams
    passed = [None] * streams
    hist = [[] for _ in range(streams)]
    hids = [[] for _ in range(streams)]
    waiting = []
    taken = 0
    total = None
    zero = jnp.zeros((rows, 2 * width), BF)
    tick = normed[:8, :128].astype(F32) * 0.0
    last = max(len(ks) for ks in lists) + 2 * (M - 1) - 2
    straight = [[] for _ in range(streams)]
    for t in range(last + 1):
        for s in range(streams):
            ks = lists[s]
            n = len(ks)
            came = got[s]
            if t < n + M - 2:
                options = [part(ks[t - p]) if 0 <= t - p < n else zero for p in range(M - 1)]
                own = choose(options + [zero])
                send = own if came is None else (own.astype(F32) + came.astype(F32)).astype(BF)
                got[s] = lax.ppermute(send, ("ctx", "mp"), inward)
            i = t - (M - 1)
            if 0 <= i < n:
                full = came.astype(F32) + part(ks[i]).astype(F32)
                g, u = full[:, :width], full[:, width:]
                hids[s].append((jax.nn.silu(g) * u).astype(BF))
            if 0 <= i < n - 1 + M - 2:
                fresh = hids[s][i] if i < n - 1 else jnp.zeros((rows, width), BF)
                send = fresh if passed[s] is None else jnp.where(place == M - 1, fresh, passed[s])
                passed[s] = lax.ppermute(send, ("ctx", "mp"), outward)
                hist[s].append(passed[s])
            if i == n - 1:
                for d in reversed(range(1, M)):
                    pairs = grid.flat([(at(a, M - 1), at(a, M - 1 - d)) for a in range(C)])
                    straight[s].append(lax.ppermute(hids[s][i], ("ctx", "mp"), pairs))
            j = i - (M - 2) - 1
            if 0 <= j < n - 1:
                waiting.append(
                    (ks[j], choose([hist[s][j + M - 2 - p] for p in range(M - 1)] + [hids[s][j]]))
                )
            if i == n + M - 3:
                waiting.append((ks[n - 1], choose(straight[s] + [hids[s][n - 1]])))
            tick = tick * 0.5
            tick = lax.optimization_barrier(tick)
            final = taken + len(waiting) == count
            waiting.sort(key=lambda kv: kv[0])
            run = bool(waiting) and waiting[-1][0] - waiting[0][0] == len(waiting) - 1
            if waiting and ((len(waiting) >= GROUP and run) or final):
                taken += len(waiting)
                k0, k1 = waiting[0][0], waiting[-1][0] + 1
                block = lax.optimization_barrier(jnp.concatenate([b for _, b in waiting], axis=1))
                waiting.clear()
                weight = down_weight[k0 * width : k1 * width]
                if final:
                    half = rows // 2
                    far = jnp.dot(block[half:], weight, preferred_element_type=F32)
                    near = jnp.dot(block[:half], weight, preferred_element_type=F32)
                    near = lax.optimization_barrier(near)
                    if total is not None:
                        far = far + total[half:]
                        near = near + total[:half]
                else:
                    piece = jnp.dot(block, weight, preferred_element_type=F32)
                    total = lax.optimization_barrier(piece if total is None else total + piece)
    return near, far, tick[0, 0]


def body(
    tokens,
    norm_gain,
    router_weight,
    query_weight,
    key_weight,
    value_weight,
    out_weight,
    mlp_gain,
    gate_weight,
    up_weight,
    down_weight,
    destination,
    kept_pos,
):
    grid = Grid()
    ctx_count, mp_count = grid.C, grid.M
    my_index = grid.c
    tok_dev = tokens.shape[0]
    kept_dev = kept_pos.shape[0]
    rows = kept_dev * ctx_count
    feature_cols = tokens.shape[1]
    feature_total = feature_cols * mp_count
    slice_cols = feature_total // ctx_count
    capacity = (3 * kept_dev // 2 + ctx_count - 1) // ctx_count
    slots_all = ctx_count * capacity
    head_dim = HEAD_DIM
    query_cols = query_weight.shape[1]
    key_cols = key_weight.shape[1]
    kv_local = key_cols // head_dim
    q_local = query_cols // head_dim
    group_size = q_local // kv_local
    peer_ids = jnp.arange(ctx_count, dtype=jnp.int32)
    is_kept = destination >= 0
    owner_ids = destination // kept_dev
    slot_ids = destination % kept_dev
    kept_order = slot_ids * ctx_count + owner_ids
    first_order = jnp.min(jnp.where(is_kept, kept_order, ctx_count * kept_dev))
    first_slots = (first_order - peer_ids + ctx_count - 1) // ctx_count
    owner_match = owner_ids[:, None] == peer_ids[None, :]
    send_index = (
        owner_ids * capacity
        + slot_ids
        - jnp.sum(jnp.where(owner_match, first_slots[None, :], 0), axis=1)
    )
    send_index = jnp.where(is_kept, send_index, slots_all)
    slot_ids_all = jnp.arange(slots_all, dtype=jnp.int32)
    takes = (slot_ids_all[:, None] == send_index[None, :]).astype(BF)
    outgoing = (
        jnp.dot(takes, tokens, preferred_element_type=F32)
        .astype(BF)
        .reshape(ctx_count, capacity, feature_cols)
    )
    positions = grid.small_gather(kept_pos.astype(F32))
    incoming = lax.all_to_all(outgoing, "ctx", split_axis=0, concat_axis=0, tiled=True).reshape(
        slots_all, feature_cols
    )
    slot_range = jnp.arange(kept_dev, dtype=jnp.int32)
    source_ids = kept_pos // tok_dev
    source_match = source_ids[:, None] == peer_ids[None, :]
    first_from = jnp.min(jnp.where(source_match, slot_range[:, None], kept_dev), axis=0)
    recv_index = (
        source_ids * capacity
        + slot_range
        - jnp.sum(jnp.where(source_match, first_from[None, :], 0), axis=1)
    )
    local_rows = incoming[recv_index]
    fits = q_local == ctx_count and kv_local == 2 and len(grid.far_bits) == 2
    pos_all = grid.xor_order(positions, my_index ^ (grid.H * grid.m)).reshape(rows)
    blocks = grid.rows_to_slices(local_rows)
    raw_share = local_rows.astype(F32)
    my_router = lax.dynamic_slice(router_weight, (grid.m * feature_cols,), (feature_cols,))
    square_part = jnp.concatenate([jnp.sum(b.astype(F32) ** 2, axis=1) for b in blocks])
    my_gain = lax.dynamic_slice(norm_gain, (my_index * slice_cols,), (slice_cols,))
    my_gain = my_gain.astype(F32)[None, :]
    scaled = jnp.concatenate([(b.astype(F32) * my_gain).astype(BF) for b in blocks], axis=0)
    softmax_scale = head_dim ** (-0.5)
    if fits:
        send_weight, keep_weight = head_weights(grid, query_weight, key_weight, value_weight)
        out_rows = jnp.concatenate(
            [
                lax.dynamic_slice(
                    out_weight, ((my_index ^ i) * head_dim, 0), (head_dim, out_weight.shape[1])
                )
                for i in grid.order
            ],
            axis=0,
        )
        send = jnp.dot(scaled, send_weight, preferred_element_type=F32).astype(BF)
        keep = jnp.dot(scaled, keep_weight, preferred_element_type=F32)
        keep = lax.optimization_barrier(keep)
        query, own, square_sum = head_reduce(grid, send, keep, square_part)
        inverse_all = lax.rsqrt(square_sum / feature_total + 1e-05)
        query = rotate(query * inverse_all[:, None], pos_all).astype(BF)
        own = own * inverse_all[:, None]
        even = grid.bit(1) == 0
        own = jnp.where(even, rotate(own, pos_all), own).astype(BF)
        other = grid.swap(own, 1)
        keys = jnp.where(even, own, other)
        values = jnp.where(even, other, own)
        allowed = pos_all[None, :] <= pos_all[:, None]
        scores = (
            lax.dot_general(query, keys, (((1,), (1,)), ((), ())), preferred_element_type=F32)
            * softmax_scale
        )
        scores = jnp.where(allowed, scores, -1e30)
        peak = jnp.max(scores, axis=-1, keepdims=True)
        weights = jnp.where(allowed, jnp.exp(scores - peak), 0.0)
        weighted = jnp.dot(weights, values.astype(F32))
        attended = (weighted / jnp.sum(weights, axis=-1, keepdims=True)).astype(BF)
        half = rows // 2
        first = grid.far_gather(attended[:half], grid.far_bits)
        second = grid.far_gather(attended[half:], grid.far_bits[::-1])
        near = jnp.concatenate(
            [jnp.concatenate([first[i], second[i]], axis=0) for i in grid.even], axis=1
        )
        span = len(grid.even) * head_dim
        partial_cols = jnp.dot(near, out_rows[:span], preferred_element_type=F32) + jnp.dot(
            grid.swap(near, 1), out_rows[span:], preferred_element_type=F32
        )
    else:
        stacked = jnp.concatenate([query_weight, key_weight, value_weight], axis=1)
        projected = jnp.dot(scaled, stacked, preferred_element_type=F32)
        mine = lax.psum_scatter(projected, "ctx", scatter_dimension=0, tiled=True)
        square_sum = lax.psum_scatter(square_part, "ctx", scatter_dimension=0, tiled=True)
        my_inverse = lax.rsqrt(square_sum / feature_total + 1e-05)
        my_pos = lax.dynamic_slice(pos_all, (my_index * kept_dev,), (kept_dev,))
        mine = mine * my_inverse[:, None]
        by_head = mine.reshape(kept_dev, q_local + 2 * kv_local, head_dim).transpose(1, 0, 2)
        queries = rotate(by_head[:q_local], my_pos).astype(BF)
        queries = queries.reshape(kv_local, group_size, kept_dev, head_dim)
        keys = rotate(by_head[q_local : q_local + kv_local], my_pos).astype(BF)
        values = by_head[q_local + kv_local :].astype(BF)
        keys = lax.all_gather(keys, "ctx", axis=1, tiled=True)
        values = lax.all_gather(values, "ctx", axis=1, tiled=True)
        allowed = pos_all[None, :] <= my_pos[:, None]
        scores = (
            jnp.einsum("hgqd,hkd->hgqk", queries, keys, preferred_element_type=F32) * softmax_scale
        )
        scores = jnp.where(allowed, scores, -1e30)
        peak = jnp.max(scores, axis=-1, keepdims=True)
        weights = jnp.where(allowed, jnp.exp(scores - peak), 0.0)
        weighted = jnp.einsum("hgqk,hkd->hgqd", weights, values.astype(F32))
        attended = weighted / jnp.sum(weights, axis=-1, keepdims=True)
        attended = attended.transpose(2, 0, 1, 3).reshape(kept_dev, query_cols).astype(BF)
        every_head = lax.all_gather(attended, "ctx", axis=0, tiled=True)
        partial_cols = jnp.dot(every_head, out_weight, preferred_element_type=F32)
    head_share = jnp.concatenate(grid.slices_to_rows(partial_cols.astype(BF)), axis=1)
    mixed_share = raw_share + head_share
    sums = grid.mp_sum(
        jnp.stack(
            [
                jnp.sum(mixed_share * mixed_share, axis=1),
                jnp.sum(raw_share * my_router.astype(F32)[None, :], axis=1),
            ]
        )
    )
    router_score = jax.nn.sigmoid(sums[1])
    second_inverse = grid.small_gather(lax.rsqrt(sums[0] / feature_total + 1e-05))
    second_inverse = jnp.concatenate([second_inverse[i] for i in grid.order])[:, None]
    second_scaled = (mixed_share * mlp_gain.astype(F32)).astype(BF)
    mid = feature_cols // 2
    every_scaled = grid.gather((second_scaled[:, :mid], second_scaled[:, mid:]))
    every_scaled = (every_scaled.astype(F32) * second_inverse).astype(BF)
    near, far, tick = feed_forward(grid, every_scaled, gate_weight, up_weight, down_weight)
    mlp_share = grid.scatter_sum(near, far)
    update = (router_score[:, None] * (head_share + mlp_share) + tick).astype(BF)
    places = (slot_ids_all[:, None] == recv_index[None, :]).astype(BF)
    returning = (
        jnp.dot(places, update, preferred_element_type=F32)
        .astype(BF)
        .reshape(ctx_count, capacity, feature_cols)
    )
    returned = lax.all_to_all(returning, "ctx", split_axis=0, concat_axis=0, tiled=True).reshape(
        slots_all, feature_cols
    )
    lands = (send_index[:, None] == slot_ids_all[None, :]).astype(BF)
    arriving = jnp.dot(lands, returned, preferred_element_type=F32)
    return (tokens.astype(F32) + arriving).astype(BF)


def solution(mesh):
    in_specs = (
        P("ctx", "mp"),
        P(),
        P(),
        P("ctx", "mp"),
        P("ctx", "mp"),
        P("ctx", "mp"),
        P("mp", "ctx"),
        P("mp"),
        P("mp", "ctx"),
        P("mp", "ctx"),
        P("ctx", "mp"),
        P("ctx"),
        P("ctx"),
    )
    out_specs = P("ctx", "mp")

    return jax.shard_map(body, mesh=mesh, in_specs=in_specs, out_specs=out_specs, check_vma=False)
```

```python
import jax
import jax.numpy as jnp
from jax import lax
from jax.sharding import PartitionSpec as P


HEAD_DIM = 128
BF = jnp.bfloat16
F32 = jnp.float32
WIDTH = 256
GROUP = 4


def rotate(values, positions):
    half_dim = values.shape[-1] // 2
    exponent = jnp.arange(half_dim, dtype=F32) * (2.0 / values.shape[-1])
    frequency = 500000.0 ** (-exponent)
    angles = positions.astype(F32)[:, None] * frequency[None, :]
    cosine = jnp.cos(angles)
    sine_part = jnp.sin(angles)
    first_half = values[..., :half_dim]
    second_half = values[..., half_dim:]
    return jnp.concatenate(
        [
            first_half * cosine - second_half * sine_part,
            second_half * cosine + first_half * sine_part,
        ],
        axis=-1,
    )


def flip_blocks(x, b):
    view = x.reshape(x.shape[0] // (2 * b), 2, b, *x.shape[1:])
    return view[:, ::-1].reshape(x.shape)


class Grid:
    def __init__(self):
        self.C = lax.axis_size("ctx")
        self.M = lax.axis_size("mp")
        self.c = lax.axis_index("ctx")
        self.m = lax.axis_index("mp")
        self.H = self.C // self.M
        self.far_bits = []
        bit = 2
        while bit < self.C:
            self.far_bits.append(bit)
            bit *= 2
        self.even = list(range(0, self.C, 2))
        self.order = self.even + [i + 1 for i in self.even]

    def bit(self, b):
        return (self.c // b) % 2

    def swap(self, x, b):
        return lax.ppermute(x, "ctx", [(i, i ^ b) for i in range(self.C)])

    def flat(self, pairs):
        return [(a * self.M + b, d * self.M + e) for (a, b), (d, e) in pairs]

    def rotate_mp(self, block_for):
        return [
            lax.ppermute(block_for(s), "mp", [(i, (i + s) % self.M) for i in range(self.M)])
            for s in range(1, self.M)
        ]

    def mp_sum(self, x):
        total = x
        for other in self.rotate_mp(lambda s: x):
            total = total + other
        return total

    def far_gather(self, x, bits):
        have = {0: x}
        for b in bits:
            keys = list(have)
            got = self.swap(jnp.stack([have[k] for k in keys]), b)
            for j, k in enumerate(keys):
                have[k ^ b] = got[j]
        return have

    def gather(self, parts):
        a = self.far_gather(parts[0], self.far_bits)
        b = self.far_gather(parts[1], self.far_bits[::-1])
        near = jnp.concatenate(
            [jnp.concatenate([a[i], b[i]], axis=1) for i in self.even], axis=0
        )
        return jnp.concatenate([near, self.swap(near, 1)], axis=0)

    def small_gather(self, x):
        out = x[None]
        b = 1
        while b < self.C:
            out = jnp.concatenate([out, self.swap(out, b)])
            b *= 2
        return out

    def xor_order(self, x, value):
        b = 1
        while b < self.C:
            x = jnp.where((value // b) % 2 == 1, flip_blocks(x, b), x)
            b *= 2
        return x

    def far_halve(self, blocks, bits):
        for b in bits:
            keep = [k for k in blocks if not k & b]
            got = self.swap(jnp.stack([blocks[k ^ b] for k in keep]).astype(BF), b)
            blocks = {k: blocks[k] + got[j].astype(F32) for j, k in enumerate(keep)}
        return blocks[0]

    def scatter_sum(self, near, far):
        half = near.shape[1] // 2
        n = near.shape[0] // len(self.even)
        near = near + self.swap(far.astype(BF), 1).astype(F32)
        parts = []
        for cols, bits in (
            (slice(0, half), self.far_bits[::-1]),
            (slice(half, None), self.far_bits),
        ):
            blocks = {i: near[j * n : (j + 1) * n, cols] for j, i in enumerate(self.even)}
            parts.append(self.far_halve(blocks, bits))
        return jnp.concatenate(parts, axis=1)

    def rows_to_slices(self, local_rows):
        n = local_rows.shape[0]
        f = local_rows.shape[1] // self.H
        payload = [
            lax.dynamic_slice(local_rows, (0, ((self.c % self.H) ^ i) * f), (n, f))
            for i in range(self.H)
        ]
        blocks = []
        for r in range(self.C):
            pairs = [
                ((a, b), (self.H * b + (a ^ r) % self.H, (a ^ r) // self.H))
                for a in range(self.C)
                for b in range(self.M)
            ]
            blocks.append(lax.ppermute(payload[r % self.H], ("ctx", "mp"), self.flat(pairs)))
        b = 1
        while b < self.H:
            swapped = self.bit(b) == 1
            blocks = [jnp.where(swapped, blocks[r ^ b], blocks[r]) for r in range(self.C)]
            b *= 2
        return blocks

    def slices_to_rows(self, partial):
        n = partial.shape[0] // self.C
        f = partial.shape[1]
        first = self.H * self.m
        full = jnp.zeros((self.C, n, f), BF)
        for r in range(self.C):
            got = lax.dynamic_slice(partial, (((self.c ^ r) ^ first) * n, 0), (n, f))
            if r:
                got = self.swap(got, r)
            full = lax.dynamic_update_slice(full, got[None], (self.c ^ r, 0, 0))

        def share(s):
            return lax.dynamic_slice(full, ((self.m + s) % self.M * self.H, 0, 0), (self.H, n, f))

        total = share(0).astype(F32)
        for got in self.rotate_mp(share):
            total = total + got.astype(F32)
        return [total[h] for h in range(self.H)]


def columns(weight, index):
    return lax.dynamic_slice(
        weight, (0, index * HEAD_DIM), (weight.shape[0], HEAD_DIM)
    )


def head_weights(grid, query_weight, key_weight, value_weight):
    group = grid.c // (grid.C // 2)
    odd = grid.bit(1) == 1
    mine = jnp.where(odd, value_weight, key_weight)
    other = jnp.where(odd, key_weight, value_weight)

    def side(near, kv):
        parts = []
        for g in range(2):
            parts += [columns(query_weight, grid.c ^ (i + near)) for i in grid.even[2 * g : 2 * g + 2]]
            parts.append(columns(kv, group ^ g))
        return jnp.concatenate(parts, axis=1)

    return side(1, other), side(0, mine)


def head_reduce(grid, send, keep, squares):
    d = HEAD_DIM
    other = grid.swap(send, 1)
    squares = squares + grid.swap(squares, 1)
    near = keep + other.astype(F32)
    half = near.shape[0] // 2
    group_bit = grid.C // 2
    side_bit = grid.far_bits[0]
    first, second = near[:half], near[half:]
    sq_a, sq_b = squares[:half], squares[half:]
    out = jnp.concatenate([second[:, d : 3 * d], second[:, 4 * d :]], axis=1).astype(BF)
    got_a = grid.swap(first[:, 3 * d :].astype(BF), group_bit).astype(F32)
    got_b = grid.swap(out, side_bit).astype(F32)
    sq_a = sq_a + grid.swap(sq_a, group_bit)
    sq_b = sq_b + grid.swap(sq_b, side_bit)
    a = first[:, : 3 * d] + got_a
    b0 = second[:, :d] + got_b[:, :d]
    bg0 = second[:, 2 * d : 3 * d] + got_b[:, d : 2 * d]
    b4 = second[:, 3 * d : 4 * d] + got_b[:, 2 * d : 3 * d]
    bg1 = second[:, 5 * d :] + got_b[:, 3 * d :]
    got_a = grid.swap(a[:, d:].astype(BF), side_bit).astype(F32)
    got_b = grid.swap(jnp.concatenate([b4, bg1], axis=1).astype(BF), group_bit).astype(F32)
    sq_a = sq_a + grid.swap(sq_a, side_bit)
    sq_b = sq_b + grid.swap(sq_b, group_bit)
    query = jnp.concatenate([a[:, :d] + got_a[:, :d], b0 + got_b[:, :d]], axis=0)
    own = jnp.concatenate([a[:, 2 * d :] + got_a[:, d:], bg0 + got_b[:, d:]], axis=0)
    return query, own, jnp.concatenate([sq_a, sq_b])


def feed_forward(grid, normed, gate_weight, up_weight, down_weight):
    C, M = grid.C, grid.M
    rows = normed.shape[0]
    hidden_cols = gate_weight.shape[1]
    width = WIDTH if hidden_cols % WIDTH == 0 else HEAD_DIM
    count = hidden_cols // width
    streams = 2
    place = jnp.where(grid.c % 2 == 1, grid.m, M - 1 - grid.m)

    def at(a, p):
        return (a, p if a % 2 == 1 else M - 1 - p)

    inward = grid.flat([(at(a, p), at(a, p + 1)) for a in range(C) for p in range(M - 1)])
    outward = grid.flat([(at(a, p + 1), at(a, p)) for a in range(C) for p in range(M - 1)])

    def choose(options):
        return lax.select_n(place, *options)

    products = {}

    def part(k):
        first = k - k % streams
        if first not in products:
            lo, hi = first * width, min(first + streams, count) * width
            g = jnp.dot(normed, gate_weight[:, lo:hi], preferred_element_type=F32).astype(BF)
            u = jnp.dot(normed, up_weight[:, lo:hi], preferred_element_type=F32).astype(BF)
            products[first] = g, u
        cols = slice((k - first) * width, (k - first + 1) * width)
        g, u = products[first]
        return jnp.concatenate([g[:, cols], u[:, cols]], axis=1)

    lists = [list(range(s, count, streams)) for s in range(streams)]
    got = [None] * streams
    passed = [None] * streams
    hist = [[] for _ in range(streams)]
    hids = [[] for _ in range(streams)]
    waiting = []
    taken = 0
    total = None
    zero = jnp.zeros((rows, 2 * width), BF)
    tick = normed[:8, :128].astype(F32) * 0.0
    last = max(len(ks) for ks in lists) + 2 * (M - 1) - 2
    straight = [[] for _ in range(streams)]
    for t in range(last + 1):
        for s in range(streams):
            ks = lists[s]
            n = len(ks)
            came = got[s]
            if t < n + M - 2:
                options = [part(ks[t - p]) if 0 <= t - p < n else zero for p in range(M - 1)]
                own = choose(options + [zero])
                send = own if came is None else (own.astype(F32) + came.astype(F32)).astype(BF)
                got[s] = lax.ppermute(send, ("ctx", "mp"), inward)
            i = t - (M - 1)
            if 0 <= i < n:
                full = came.astype(F32) + part(ks[i]).astype(F32)
                g, u = full[:, :width], full[:, width:]
                hids[s].append((jax.nn.silu(g) * u).astype(BF))
            if 0 <= i < n - 1 + M - 2:
                fresh = hids[s][i] if i < n - 1 else jnp.zeros((rows, width), BF)
                send = fresh if passed[s] is None else jnp.where(place == M - 1, fresh, passed[s])
                passed[s] = lax.ppermute(send, ("ctx", "mp"), outward)
                hist[s].append(passed[s])
            if i == n - 1:
                for d in reversed(range(1, M)):
                    pairs = grid.flat([(at(a, M - 1), at(a, M - 1 - d)) for a in range(C)])
                    straight[s].append(lax.ppermute(hids[s][i], ("ctx", "mp"), pairs))
            j = i - (M - 2) - 1
            if 0 <= j < n - 1:
                waiting.append(
                    (ks[j], choose([hist[s][j + M - 2 - p] for p in range(M - 1)] + [hids[s][j]]))
                )
            if i == n + M - 3:
                waiting.append((ks[n - 1], choose(straight[s] + [hids[s][n - 1]])))
            tick = tick * 0.5
            tick = lax.optimization_barrier(tick)
            final = taken + len(waiting) == count
            waiting.sort(key=lambda kv: kv[0])
            run = bool(waiting) and waiting[-1][0] - waiting[0][0] == len(waiting) - 1
            if waiting and ((len(waiting) >= GROUP and run) or final):
                taken += len(waiting)
                k0, k1 = waiting[0][0], waiting[-1][0] + 1
                block = lax.optimization_barrier(jnp.concatenate([b for _, b in waiting], axis=1))
                waiting.clear()
                weight = down_weight[k0 * width : k1 * width]
                if final:
                    half = rows // 2
                    far = jnp.dot(block[half:], weight, preferred_element_type=F32)
                    near = jnp.dot(block[:half], weight, preferred_element_type=F32)
                    near = lax.optimization_barrier(near)
                    if total is not None:
                        far = far + total[half:]
                        near = near + total[:half]
                else:
                    piece = jnp.dot(block, weight, preferred_element_type=F32)
                    total = lax.optimization_barrier(piece if total is None else total + piece)
    return near, far, tick[0, 0]


def body(
    tokens,
    norm_gain,
    router_weight,
    query_weight,
    key_weight,
    value_weight,
    out_weight,
    mlp_gain,
    gate_weight,
    up_weight,
    down_weight,
    destination,
    kept_pos,
):
    grid = Grid()
    ctx_count, mp_count = grid.C, grid.M
    my_index = grid.c
    tok_dev = tokens.shape[0]
    kept_dev = kept_pos.shape[0]
    rows = kept_dev * ctx_count
    feature_cols = tokens.shape[1]
    feature_total = feature_cols * mp_count
    slice_cols = feature_total // ctx_count
    capacity = (3 * kept_dev // 2 + ctx_count - 1) // ctx_count
    slots_all = ctx_count * capacity
    head_dim = HEAD_DIM
    query_cols = query_weight.shape[1]
    key_cols = key_weight.shape[1]
    kv_local = key_cols // head_dim
    q_local = query_cols // head_dim
    group_size = q_local // kv_local
    peer_ids = jnp.arange(ctx_count, dtype=jnp.int32)
    is_kept = destination >= 0
    owner_ids = destination // kept_dev
    slot_ids = destination % kept_dev
    kept_order = slot_ids * ctx_count + owner_ids
    first_order = jnp.min(jnp.where(is_kept, kept_order, ctx_count * kept_dev))
    first_slots = (first_order - peer_ids + ctx_count - 1) // ctx_count
    owner_match = owner_ids[:, None] == peer_ids[None, :]
    send_index = (
        owner_ids * capacity
        + slot_ids
        - jnp.sum(jnp.where(owner_match, first_slots[None, :], 0), axis=1)
    )
    send_index = jnp.where(is_kept, send_index, slots_all)
    slot_ids_all = jnp.arange(slots_all, dtype=jnp.int32)
    takes = (slot_ids_all[:, None] == send_index[None, :]).astype(BF)
    outgoing = (
        jnp.dot(takes, tokens, preferred_element_type=F32)
        .astype(BF)
        .reshape(ctx_count, capacity, feature_cols)
    )
    positions = grid.small_gather(kept_pos.astype(F32))
    incoming = lax.all_to_all(outgoing, "ctx", split_axis=0, concat_axis=0, tiled=True).reshape(
        slots_all, feature_cols
    )
    slot_range = jnp.arange(kept_dev, dtype=jnp.int32)
    source_ids = kept_pos // tok_dev
    source_match = source_ids[:, None] == peer_ids[None, :]
    first_from = jnp.min(jnp.where(source_match, slot_range[:, None], kept_dev), axis=0)
    recv_index = (
        source_ids * capacity
        + slot_range
        - jnp.sum(jnp.where(source_match, first_from[None, :], 0), axis=1)
    )
    local_rows = incoming[recv_index]
    fits = q_local == ctx_count and kv_local == 2 and len(grid.far_bits) == 2
    pos_all = grid.xor_order(positions, my_index ^ (grid.H * grid.m)).reshape(rows)
    blocks = grid.rows_to_slices(local_rows)
    raw_share = local_rows.astype(F32)
    my_router = lax.dynamic_slice(router_weight, (grid.m * feature_cols,), (feature_cols,))
    square_part = jnp.concatenate([jnp.sum(b.astype(F32) ** 2, axis=1) for b in blocks])
    my_gain = lax.dynamic_slice(norm_gain, (my_index * slice_cols,), (slice_cols,))
    my_gain = my_gain.astype(F32)[None, :]
    scaled = jnp.concatenate([(b.astype(F32) * my_gain).astype(BF) for b in blocks], axis=0)
    softmax_scale = head_dim ** (-0.5)
    if fits:
        send_weight, keep_weight = head_weights(grid, query_weight, key_weight, value_weight)
        out_rows = jnp.concatenate(
            [
                lax.dynamic_slice(
                    out_weight, ((my_index ^ i) * head_dim, 0), (head_dim, out_weight.shape[1])
                )
                for i in grid.order
            ],
            axis=0,
        )
        send = jnp.dot(scaled, send_weight, preferred_element_type=F32).astype(BF)
        keep = jnp.dot(scaled, keep_weight, preferred_element_type=F32)
        keep = lax.optimization_barrier(keep)
        query, own, square_sum = head_reduce(grid, send, keep, square_part)
        inverse_all = lax.rsqrt(square_sum / feature_total + 1e-05)
        query = rotate(query * inverse_all[:, None], pos_all).astype(BF)
        own = own * inverse_all[:, None]
        even = grid.bit(1) == 0
        own = jnp.where(even, rotate(own, pos_all), own).astype(BF)
        other = grid.swap(own, 1)
        keys = jnp.where(even, own, other)
        values = jnp.where(even, other, own)
        allowed = pos_all[None, :] <= pos_all[:, None]
        scores = (
            lax.dot_general(query, keys, (((1,), (1,)), ((), ())), preferred_element_type=F32)
            * softmax_scale
        )
        scores = jnp.where(allowed, scores, -1e30)
        peak = jnp.max(scores, axis=-1, keepdims=True)
        weights = jnp.where(allowed, jnp.exp(scores - peak), 0.0)
        weighted = jnp.dot(weights, values.astype(F32))
        attended = (weighted / jnp.sum(weights, axis=-1, keepdims=True)).astype(BF)
        half = rows // 2
        first = grid.far_gather(attended[:half], grid.far_bits)
        second = grid.far_gather(attended[half:], grid.far_bits[::-1])
        near = jnp.concatenate(
            [jnp.concatenate([first[i], second[i]], axis=0) for i in grid.even], axis=1
        )
        span = len(grid.even) * head_dim
        partial_cols = jnp.dot(near, out_rows[:span], preferred_element_type=F32) + jnp.dot(
            grid.swap(near, 1), out_rows[span:], preferred_element_type=F32
        )
    else:
        stacked = jnp.concatenate([query_weight, key_weight, value_weight], axis=1)
        projected = jnp.dot(scaled, stacked, preferred_element_type=F32)
        mine = lax.psum_scatter(projected, "ctx", scatter_dimension=0, tiled=True)
        square_sum = lax.psum_scatter(square_part, "ctx", scatter_dimension=0, tiled=True)
        my_inverse = lax.rsqrt(square_sum / feature_total + 1e-05)
        my_pos = lax.dynamic_slice(pos_all, (my_index * kept_dev,), (kept_dev,))
        mine = mine * my_inverse[:, None]
        by_head = mine.reshape(kept_dev, q_local + 2 * kv_local, head_dim).transpose(1, 0, 2)
        queries = rotate(by_head[:q_local], my_pos).astype(BF)
        queries = queries.reshape(kv_local, group_size, kept_dev, head_dim)
        keys = rotate(by_head[q_local : q_local + kv_local], my_pos).astype(BF)
        values = by_head[q_local + kv_local :].astype(BF)
        keys = lax.all_gather(keys, "ctx", axis=1, tiled=True)
        values = lax.all_gather(values, "ctx", axis=1, tiled=True)
        allowed = pos_all[None, :] <= my_pos[:, None]
        scores = (
            jnp.einsum("hgqd,hkd->hgqk", queries, keys, preferred_element_type=F32) * softmax_scale
        )
        scores = jnp.where(allowed, scores, -1e30)
        peak = jnp.max(scores, axis=-1, keepdims=True)
        weights = jnp.where(allowed, jnp.exp(scores - peak), 0.0)
        weighted = jnp.einsum("hgqk,hkd->hgqd", weights, values.astype(F32))
        attended = weighted / jnp.sum(weights, axis=-1, keepdims=True)
        attended = attended.transpose(2, 0, 1, 3).reshape(kept_dev, query_cols).astype(BF)
        every_head = lax.all_gather(attended, "ctx", axis=0, tiled=True)
        partial_cols = jnp.dot(every_head, out_weight, preferred_element_type=F32)
    head_share = jnp.concatenate(grid.slices_to_rows(partial_cols.astype(BF)), axis=1)
    mixed_share = raw_share + head_share
    sums = grid.mp_sum(
        jnp.stack(
            [
                jnp.sum(mixed_share * mixed_share, axis=1),
                jnp.sum(raw_share * my_router.astype(F32)[None, :], axis=1),
            ]
        )
    )
    router_score = jax.nn.sigmoid(sums[1])
    second_inverse = grid.small_gather(lax.rsqrt(sums[0] / feature_total + 1e-05))
    second_inverse = jnp.concatenate([second_inverse[i] for i in grid.order])[:, None]
    second_scaled = (mixed_share * mlp_gain.astype(F32)).astype(BF)
    mid = feature_cols // 2
    every_scaled = grid.gather((second_scaled[:, :mid], second_scaled[:, mid:]))
    every_scaled = (every_scaled.astype(F32) * second_inverse).astype(BF)
    near, far, tick = feed_forward(grid, every_scaled, gate_weight, up_weight, down_weight)
    mlp_share = grid.scatter_sum(near, far)
    update = (router_score[:, None] * (head_share + mlp_share) + tick).astype(BF)
    places = (slot_ids_all[:, None] == recv_index[None, :]).astype(BF)
    returning = (
        jnp.dot(places, update, preferred_element_type=F32)
        .astype(BF)
        .reshape(ctx_count, capacity, feature_cols)
    )
    returned = lax.all_to_all(returning, "ctx", split_axis=0, concat_axis=0, tiled=True).reshape(
        slots_all, feature_cols
    )
    lands = (send_index[:, None] == slot_ids_all[None, :]).astype(BF)
    arriving = jnp.dot(lands, returned, preferred_element_type=F32)
    return (tokens.astype(F32) + arriving).astype(BF)


def solution(mesh):
    in_specs = (
        P("ctx", "mp"),
        P(),
        P(),
        P("ctx", "mp"),
        P("ctx", "mp"),
        P("ctx", "mp"),
        P("mp", "ctx"),
        P("mp"),
        P("mp", "ctx"),
        P("mp", "ctx"),
        P("ctx", "mp"),
        P("ctx"),
        P("ctx"),
    )
    out_specs = P("ctx", "mp")

    return jax.shard_map(body, mesh=mesh, in_specs=in_specs, out_specs=out_specs, check_vma=False)
```

```python
import jax
import jax.numpy as jnp
from jax import lax
from jax.sharding import PartitionSpec as P


HEAD_DIM = 128
BF = jnp.bfloat16
F32 = jnp.float32
WIDTH = 256
GROUP = 4


def rotate(values, positions):
    half_dim = values.shape[-1] // 2
    exponent = jnp.arange(half_dim, dtype=F32) * (2.0 / values.shape[-1])
    frequency = 500000.0 ** (-exponent)
    angles = positions.astype(F32)[:, None] * frequency[None, :]
    cosine = jnp.cos(angles)
    sine_part = jnp.sin(angles)
    first_half = values[..., :half_dim]
    second_half = values[..., half_dim:]
    return jnp.concatenate(
        [
            first_half * cosine - second_half * sine_part,
            second_half * cosine + first_half * sine_part,
        ],
        axis=-1,
    )


def flip_blocks(x, b):
    view = x.reshape(x.shape[0] // (2 * b), 2, b, *x.shape[1:])
    return view[:, ::-1].reshape(x.shape)


class Grid:
    def __init__(self):
        self.C = lax.axis_size("ctx")
        self.M = lax.axis_size("mp")
        self.c = lax.axis_index("ctx")
        self.m = lax.axis_index("mp")
        self.H = self.C // self.M
        self.far_bits = []
        bit = 2
        while bit < self.C:
            self.far_bits.append(bit)
            bit *= 2
        self.even = list(range(0, self.C, 2))
        self.order = self.even + [i + 1 for i in self.even]

    def bit(self, b):
        return (self.c // b) % 2

    def swap(self, x, b):
        return lax.ppermute(x, "ctx", [(i, i ^ b) for i in range(self.C)])

    def flat(self, pairs):
        return [(a * self.M + b, d * self.M + e) for (a, b), (d, e) in pairs]

    def rotate_mp(self, block_for):
        return [
            lax.ppermute(block_for(s), "mp", [(i, (i + s) % self.M) for i in range(self.M)])
            for s in range(1, self.M)
        ]

    def mp_sum(self, x):
        total = x
        for other in self.rotate_mp(lambda s: x):
            total = total + other
        return total

    def far_gather(self, x, bits):
        have = {0: x}
        for b in bits:
            keys = list(have)
            got = self.swap(jnp.stack([have[k] for k in keys]), b)
            for j, k in enumerate(keys):
                have[k ^ b] = got[j]
        return have

    def gather(self, parts):
        a = self.far_gather(parts[0], self.far_bits)
        b = self.far_gather(parts[1], self.far_bits[::-1])
        near = jnp.concatenate(
            [jnp.concatenate([a[i], b[i]], axis=1) for i in self.even], axis=0
        )
        return jnp.concatenate([near, self.swap(near, 1)], axis=0)

    def small_gather(self, x):
        out = x[None]
        b = 1
        while b < self.C:
            out = jnp.concatenate([out, self.swap(out, b)])
            b *= 2
        return out

    def xor_order(self, x, value):
        b = 1
        while b < self.C:
            x = jnp.where((value // b) % 2 == 1, flip_blocks(x, b), x)
            b *= 2
        return x

    def far_halve(self, blocks, bits):
        for b in bits:
            keep = [k for k in blocks if not k & b]
            got = self.swap(jnp.stack([blocks[k ^ b] for k in keep]).astype(BF), b)
            blocks = {k: blocks[k] + got[j].astype(F32) for j, k in enumerate(keep)}
        return blocks[0]

    def scatter_sum(self, near, far):
        half = near.shape[1] // 2
        n = near.shape[0] // len(self.even)
        near = near + self.swap(far.astype(BF), 1).astype(F32)
        parts = []
        for cols, bits in (
            (slice(0, half), self.far_bits[::-1]),
            (slice(half, None), self.far_bits),
        ):
            blocks = {i: near[j * n : (j + 1) * n, cols] for j, i in enumerate(self.even)}
            parts.append(self.far_halve(blocks, bits))
        return jnp.concatenate(parts, axis=1)

    def rows_to_slices(self, local_rows):
        n = local_rows.shape[0]
        f = local_rows.shape[1] // self.H
        payload = [
            lax.dynamic_slice(local_rows, (0, ((self.c % self.H) ^ i) * f), (n, f))
            for i in range(self.H)
        ]
        blocks = []
        for r in range(self.C):
            pairs = [
                ((a, b), (self.H * b + (a ^ r) % self.H, (a ^ r) // self.H))
                for a in range(self.C)
                for b in range(self.M)
            ]
            blocks.append(lax.ppermute(payload[r % self.H], ("ctx", "mp"), self.flat(pairs)))
        b = 1
        while b < self.H:
            swapped = self.bit(b) == 1
            blocks = [jnp.where(swapped, blocks[r ^ b], blocks[r]) for r in range(self.C)]
            b *= 2
        return blocks

    def slices_to_rows(self, partial):
        n = partial.shape[0] // self.C
        f = partial.shape[1]
        first = self.H * self.m
        full = jnp.zeros((self.C, n, f), BF)
        for r in range(self.C):
            got = lax.dynamic_slice(partial, (((self.c ^ r) ^ first) * n, 0), (n, f))
            if r:
                got = self.swap(got, r)
            full = lax.dynamic_update_slice(full, got[None], (self.c ^ r, 0, 0))

        def share(s):
            return lax.dynamic_slice(full, ((self.m + s) % self.M * self.H, 0, 0), (self.H, n, f))

        total = share(0).astype(F32)
        for got in self.rotate_mp(share):
            total = total + got.astype(F32)
        return [total[h] for h in range(self.H)]


def columns(weight, index):
    return lax.dynamic_slice(
        weight, (0, index * HEAD_DIM), (weight.shape[0], HEAD_DIM)
    )


def head_weights(grid, query_weight, key_weight, value_weight):
    group = grid.c // (grid.C // 2)
    odd = grid.bit(1) == 1
    mine = jnp.where(odd, value_weight, key_weight)
    other = jnp.where(odd, key_weight, value_weight)

    def side(near, kv):
        parts = []
        for g in range(2):
            parts += [columns(query_weight, grid.c ^ (i + near)) for i in grid.even[2 * g : 2 * g + 2]]
            parts.append(columns(kv, group ^ g))
        return jnp.concatenate(parts, axis=1)

    return side(1, other), side(0, mine)


def head_reduce(grid, send, keep, squares):
    d = HEAD_DIM
    other = grid.swap(send, 1)
    squares = squares + grid.swap(squares, 1)
    near = keep + other.astype(F32)
    half = near.shape[0] // 2
    group_bit = grid.C // 2
    side_bit = grid.far_bits[0]
    first, second = near[:half], near[half:]
    sq_a, sq_b = squares[:half], squares[half:]
    out = jnp.concatenate([second[:, d : 3 * d], second[:, 4 * d :]], axis=1).astype(BF)
    got_a = grid.swap(first[:, 3 * d :].astype(BF), group_bit).astype(F32)
    got_b = grid.swap(out, side_bit).astype(F32)
    sq_a = sq_a + grid.swap(sq_a, group_bit)
    sq_b = sq_b + grid.swap(sq_b, side_bit)
    a = first[:, : 3 * d] + got_a
    b0 = second[:, :d] + got_b[:, :d]
    bg0 = second[:, 2 * d : 3 * d] + got_b[:, d : 2 * d]
    b4 = second[:, 3 * d : 4 * d] + got_b[:, 2 * d : 3 * d]
    bg1 = second[:, 5 * d :] + got_b[:, 3 * d :]
    got_a = grid.swap(a[:, d:].astype(BF), side_bit).astype(F32)
    got_b = grid.swap(jnp.concatenate([b4, bg1], axis=1).astype(BF), group_bit).astype(F32)
    sq_a = sq_a + grid.swap(sq_a, side_bit)
    sq_b = sq_b + grid.swap(sq_b, group_bit)
    query = jnp.concatenate([a[:, :d] + got_a[:, :d], b0 + got_b[:, :d]], axis=0)
    own = jnp.concatenate([a[:, 2 * d :] + got_a[:, d:], bg0 + got_b[:, d:]], axis=0)
    return query, own, jnp.concatenate([sq_a, sq_b])


def feed_forward(grid, normed, gate_weight, up_weight, down_weight):
    C, M = grid.C, grid.M
    rows = normed.shape[0]
    hidden_cols = gate_weight.shape[1]
    width = WIDTH if hidden_cols % WIDTH == 0 else HEAD_DIM
    count = hidden_cols // width
    streams = 2
    place = jnp.where(grid.c % 2 == 1, grid.m, M - 1 - grid.m)

    def at(a, p):
        return (a, p if a % 2 == 1 else M - 1 - p)

    inward = grid.flat([(at(a, p), at(a, p + 1)) for a in range(C) for p in range(M - 1)])
    outward = grid.flat([(at(a, p + 1), at(a, p)) for a in range(C) for p in range(M - 1)])

    def choose(options):
        return lax.select_n(place, *options)

    products = {}

    def part(k):
        alone = k < streams
        first = k if alone else k - k % streams
        if first not in products:
            lo, hi = first * width, min(first + (1 if alone else streams), count) * width
            g = jnp.dot(normed, gate_weight[:, lo:hi], preferred_element_type=F32).astype(BF)
            u = jnp.dot(normed, up_weight[:, lo:hi], preferred_element_type=F32).astype(BF)
            products[first] = g, u
        cols = slice((k - first) * width, (k - first + 1) * width)
        g, u = products[first]
        return jnp.concatenate([g[:, cols], u[:, cols]], axis=1)

    lists = [list(range(s, count, streams)) for s in range(streams)]
    got = [None] * streams
    passed = [None] * streams
    hist = [[] for _ in range(streams)]
    hids = [[] for _ in range(streams)]
    waiting = []
    taken = 0
    total = None
    zero = jnp.zeros((rows, 2 * width), BF)
    tick = normed[:8, :128].astype(F32) * 0.0
    last = max(len(ks) for ks in lists) + 2 * (M - 1) - 2
    straight = [[] for _ in range(streams)]
    for t in range(last + 1):
        for s in range(streams):
            ks = lists[s]
            n = len(ks)
            came = got[s]
            if t < n + M - 2:
                options = [part(ks[t - p]) if 0 <= t - p < n else zero for p in range(M - 1)]
                own = choose(options + [zero])
                send = own if came is None else (own.astype(F32) + came.astype(F32)).astype(BF)
                got[s] = lax.ppermute(send, ("ctx", "mp"), inward)
            i = t - (M - 1)
            if 0 <= i < n:
                full = came.astype(F32) + part(ks[i]).astype(F32)
                g, u = full[:, :width], full[:, width:]
                hids[s].append((jax.nn.silu(g) * u).astype(BF))
            if 0 <= i < n - 1 + M - 2:
                fresh = hids[s][i] if i < n - 1 else jnp.zeros((rows, width), BF)
                send = fresh if passed[s] is None else jnp.where(place == M - 1, fresh, passed[s])
                passed[s] = lax.ppermute(send, ("ctx", "mp"), outward)
                hist[s].append(passed[s])
            if i == n - 1:
                for d in reversed(range(1, M)):
                    pairs = grid.flat([(at(a, M - 1), at(a, M - 1 - d)) for a in range(C)])
                    straight[s].append(lax.ppermute(hids[s][i], ("ctx", "mp"), pairs))
            j = i - (M - 2) - 1
            if 0 <= j < n - 1:
                waiting.append(
                    (ks[j], choose([hist[s][j + M - 2 - p] for p in range(M - 1)] + [hids[s][j]]))
                )
            if i == n + M - 3:
                waiting.append((ks[n - 1], choose(straight[s] + [hids[s][n - 1]])))
            tick = tick * 0.5
            tick = lax.optimization_barrier(tick)
            final = taken + len(waiting) == count
            waiting.sort(key=lambda kv: kv[0])
            run = bool(waiting) and waiting[-1][0] - waiting[0][0] == len(waiting) - 1
            if waiting and ((len(waiting) >= GROUP and run) or final):
                taken += len(waiting)
                k0, k1 = waiting[0][0], waiting[-1][0] + 1
                block = lax.optimization_barrier(jnp.concatenate([b for _, b in waiting], axis=1))
                waiting.clear()
                weight = down_weight[k0 * width : k1 * width]
                if final:
                    half = rows // 2
                    far = jnp.dot(block[half:], weight, preferred_element_type=F32)
                    near = jnp.dot(block[:half], weight, preferred_element_type=F32)
                    near = lax.optimization_barrier(near)
                    if total is not None:
                        far = far + total[half:]
                        near = near + total[:half]
                else:
                    piece = jnp.dot(block, weight, preferred_element_type=F32)
                    total = lax.optimization_barrier(piece if total is None else total + piece)
    return near, far, tick[0, 0]


def body(
    tokens,
    norm_gain,
    router_weight,
    query_weight,
    key_weight,
    value_weight,
    out_weight,
    mlp_gain,
    gate_weight,
    up_weight,
    down_weight,
    destination,
    kept_pos,
):
    grid = Grid()
    ctx_count, mp_count = grid.C, grid.M
    my_index = grid.c
    tok_dev = tokens.shape[0]
    kept_dev = kept_pos.shape[0]
    rows = kept_dev * ctx_count
    feature_cols = tokens.shape[1]
    feature_total = feature_cols * mp_count
    slice_cols = feature_total // ctx_count
    capacity = (3 * kept_dev // 2 + ctx_count - 1) // ctx_count
    slots_all = ctx_count * capacity
    head_dim = HEAD_DIM
    query_cols = query_weight.shape[1]
    key_cols = key_weight.shape[1]
    kv_local = key_cols // head_dim
    q_local = query_cols // head_dim
    group_size = q_local // kv_local
    peer_ids = jnp.arange(ctx_count, dtype=jnp.int32)
    is_kept = destination >= 0
    owner_ids = destination // kept_dev
    slot_ids = destination % kept_dev
    kept_order = slot_ids * ctx_count + owner_ids
    first_order = jnp.min(jnp.where(is_kept, kept_order, ctx_count * kept_dev))
    first_slots = (first_order - peer_ids + ctx_count - 1) // ctx_count
    owner_match = owner_ids[:, None] == peer_ids[None, :]
    send_index = (
        owner_ids * capacity
        + slot_ids
        - jnp.sum(jnp.where(owner_match, first_slots[None, :], 0), axis=1)
    )
    send_index = jnp.where(is_kept, send_index, slots_all)
    slot_ids_all = jnp.arange(slots_all, dtype=jnp.int32)
    takes = (slot_ids_all[:, None] == send_index[None, :]).astype(BF)
    outgoing = (
        jnp.dot(takes, tokens, preferred_element_type=F32)
        .astype(BF)
        .reshape(ctx_count, capacity, feature_cols)
    )
    positions = grid.small_gather(kept_pos.astype(F32))
    incoming = lax.all_to_all(outgoing, "ctx", split_axis=0, concat_axis=0, tiled=True).reshape(
        slots_all, feature_cols
    )
    slot_range = jnp.arange(kept_dev, dtype=jnp.int32)
    source_ids = kept_pos // tok_dev
    source_match = source_ids[:, None] == peer_ids[None, :]
    first_from = jnp.min(jnp.where(source_match, slot_range[:, None], kept_dev), axis=0)
    recv_index = (
        source_ids * capacity
        + slot_range
        - jnp.sum(jnp.where(source_match, first_from[None, :], 0), axis=1)
    )
    local_rows = incoming[recv_index]
    fits = q_local == ctx_count and kv_local == 2 and len(grid.far_bits) == 2
    pos_all = grid.xor_order(positions, my_index ^ (grid.H * grid.m)).reshape(rows)
    blocks = grid.rows_to_slices(local_rows)
    raw_share = local_rows.astype(F32)
    my_router = lax.dynamic_slice(router_weight, (grid.m * feature_cols,), (feature_cols,))
    square_part = jnp.concatenate([jnp.sum(b.astype(F32) ** 2, axis=1) for b in blocks])
    my_gain = lax.dynamic_slice(norm_gain, (my_index * slice_cols,), (slice_cols,))
    my_gain = my_gain.astype(F32)[None, :]
    scaled = jnp.concatenate([(b.astype(F32) * my_gain).astype(BF) for b in blocks], axis=0)
    softmax_scale = head_dim ** (-0.5)
    if fits:
        send_weight, keep_weight = head_weights(grid, query_weight, key_weight, value_weight)
        out_rows = jnp.concatenate(
            [
                lax.dynamic_slice(
                    out_weight, ((my_index ^ i) * head_dim, 0), (head_dim, out_weight.shape[1])
                )
                for i in grid.order
            ],
            axis=0,
        )
        send = jnp.dot(scaled, send_weight, preferred_element_type=F32).astype(BF)
        keep = jnp.dot(scaled, keep_weight, preferred_element_type=F32)
        keep = lax.optimization_barrier(keep)
        query, own, square_sum = head_reduce(grid, send, keep, square_part)
        inverse_all = lax.rsqrt(square_sum / feature_total + 1e-05)
        query = rotate(query * inverse_all[:, None], pos_all).astype(BF)
        own = own * inverse_all[:, None]
        even = grid.bit(1) == 0
        own = jnp.where(even, rotate(own, pos_all), own).astype(BF)
        other = grid.swap(own, 1)
        keys = jnp.where(even, own, other)
        values = jnp.where(even, other, own)
        allowed = pos_all[None, :] <= pos_all[:, None]
        scores = (
            lax.dot_general(query, keys, (((1,), (1,)), ((), ())), preferred_element_type=F32)
            * softmax_scale
        )
        scores = jnp.where(allowed, scores, -1e30)
        peak = jnp.max(scores, axis=-1, keepdims=True)
        weights = jnp.where(allowed, jnp.exp(scores - peak), 0.0)
        weighted = jnp.dot(weights, values.astype(F32))
        attended = (weighted / jnp.sum(weights, axis=-1, keepdims=True)).astype(BF)
        half = rows // 2
        first = grid.far_gather(attended[:half], grid.far_bits)
        second = grid.far_gather(attended[half:], grid.far_bits[::-1])
        near = jnp.concatenate(
            [jnp.concatenate([first[i], second[i]], axis=0) for i in grid.even], axis=1
        )
        span = len(grid.even) * head_dim
        partial_cols = jnp.dot(near, out_rows[:span], preferred_element_type=F32) + jnp.dot(
            grid.swap(near, 1), out_rows[span:], preferred_element_type=F32
        )
    else:
        stacked = jnp.concatenate([query_weight, key_weight, value_weight], axis=1)
        projected = jnp.dot(scaled, stacked, preferred_element_type=F32)
        mine = lax.psum_scatter(projected, "ctx", scatter_dimension=0, tiled=True)
        square_sum = lax.psum_scatter(square_part, "ctx", scatter_dimension=0, tiled=True)
        my_inverse = lax.rsqrt(square_sum / feature_total + 1e-05)
        my_pos = lax.dynamic_slice(pos_all, (my_index * kept_dev,), (kept_dev,))
        mine = mine * my_inverse[:, None]
        by_head = mine.reshape(kept_dev, q_local + 2 * kv_local, head_dim).transpose(1, 0, 2)
        queries = rotate(by_head[:q_local], my_pos).astype(BF)
        queries = queries.reshape(kv_local, group_size, kept_dev, head_dim)
        keys = rotate(by_head[q_local : q_local + kv_local], my_pos).astype(BF)
        values = by_head[q_local + kv_local :].astype(BF)
        keys = lax.all_gather(keys, "ctx", axis=1, tiled=True)
        values = lax.all_gather(values, "ctx", axis=1, tiled=True)
        allowed = pos_all[None, :] <= my_pos[:, None]
        scores = (
            jnp.einsum("hgqd,hkd->hgqk", queries, keys, preferred_element_type=F32) * softmax_scale
        )
        scores = jnp.where(allowed, scores, -1e30)
        peak = jnp.max(scores, axis=-1, keepdims=True)
        weights = jnp.where(allowed, jnp.exp(scores - peak), 0.0)
        weighted = jnp.einsum("hgqk,hkd->hgqd", weights, values.astype(F32))
        attended = weighted / jnp.sum(weights, axis=-1, keepdims=True)
        attended = attended.transpose(2, 0, 1, 3).reshape(kept_dev, query_cols).astype(BF)
        every_head = lax.all_gather(attended, "ctx", axis=0, tiled=True)
        partial_cols = jnp.dot(every_head, out_weight, preferred_element_type=F32)
    head_share = jnp.concatenate(grid.slices_to_rows(partial_cols.astype(BF)), axis=1)
    mixed_share = raw_share + head_share
    sums = grid.mp_sum(
        jnp.stack(
            [
                jnp.sum(mixed_share * mixed_share, axis=1),
                jnp.sum(raw_share * my_router.astype(F32)[None, :], axis=1),
            ]
        )
    )
    router_score = jax.nn.sigmoid(sums[1])
    second_inverse = grid.small_gather(lax.rsqrt(sums[0] / feature_total + 1e-05))
    second_inverse = jnp.concatenate([second_inverse[i] for i in grid.order])[:, None]
    second_scaled = (mixed_share * mlp_gain.astype(F32)).astype(BF)
    mid = feature_cols // 2
    every_scaled = grid.gather((second_scaled[:, :mid], second_scaled[:, mid:]))
    every_scaled = (every_scaled.astype(F32) * second_inverse).astype(BF)
    near, far, tick = feed_forward(grid, every_scaled, gate_weight, up_weight, down_weight)
    mlp_share = grid.scatter_sum(near, far)
    update = (router_score[:, None] * (head_share + mlp_share) + tick).astype(BF)
    places = (slot_ids_all[:, None] == recv_index[None, :]).astype(BF)
    returning = (
        jnp.dot(places, update, preferred_element_type=F32)
        .astype(BF)
        .reshape(ctx_count, capacity, feature_cols)
    )
    returned = lax.all_to_all(returning, "ctx", split_axis=0, concat_axis=0, tiled=True).reshape(
        slots_all, feature_cols
    )
    lands = (send_index[:, None] == slot_ids_all[None, :]).astype(BF)
    arriving = jnp.dot(lands, returned, preferred_element_type=F32)
    return (tokens.astype(F32) + arriving).astype(BF)


def solution(mesh):
    in_specs = (
        P("ctx", "mp"),
        P(),
        P(),
        P("ctx", "mp"),
        P("ctx", "mp"),
        P("ctx", "mp"),
        P("mp", "ctx"),
        P("mp"),
        P("mp", "ctx"),
        P("mp", "ctx"),
        P("ctx", "mp"),
        P("ctx"),
        P("ctx"),
    )
    out_specs = P("ctx", "mp")

    return jax.shard_map(body, mesh=mesh, in_specs=in_specs, out_specs=out_specs, check_vma=False)
```
